256 devices in a mesh: batch: 32 (over y, x, core), rows: 8 (over z).
Axes of the slice: x: 4, y: 4, z: 8, core: 2. Of those that a mesh axis runs over, the one named last changes fastest.
Arguments:
- fine_level: bfloat16 [32, 64, 192, 384], P('batch', 'rows'), may hold values from -40 to 40
- middle_level: bfloat16 [32, 32, 96, 384], P('batch', 'rows'), may hold values from -40 to 40
- coarse_level: bfloat16 [32, 16, 48, 384], P('batch', 'rows'), may hold values from -40 to 40
- two_input_weights: float32 [2, 3, 2], replicated, may hold values from 0.5 to 2
- three_input_weights: float32 [2, 3], replicated, may hold values from 0.5 to 2
- depthwise: bfloat16 [2, 4, 3, 3, 384], replicated, may hold values from -2 to 2
- pointwise: bfloat16 [2, 4, 384, 384], replicated, may hold values from -0.3125 to 0.3125
- bn_gain: float32 [2, 4, 384], replicated, may hold values from 0.5 to 1.5
- bn_bias: float32 [2, 4, 384], replicated, may hold values from -3 to 3
Outputs:
- fine_result: bfloat16 [32, 64, 192, 384], P('batch', 'rows')
- middle_result: bfloat16 [32, 32, 96, 384], P('batch', 'rows')
- coarse_result: bfloat16 [32, 16, 48, 384], P('batch', 'rows')
The draws below stay inside these ranges and needn't reach their ends.
All inputs are finite; a program needn't handle non-finite values.
Results may differ from the reference program's by a relative error of at most 0.025.
Values may be sent and summed in bfloat16 or wider, within the bound.
A program may use at most 64 MiB of HBM per device.

```python
import math
import jax
import jax.numpy as jnp
from jax import lax

C = 384
LAYERS = 2
COLS = 192
COLS_MID = 96
COLS_TOP = 48
HEIGHT = 64
HEIGHT_MID = 32
HEIGHT_TOP = 16
IMAGES = 32


def level_draw(key, height, width):
    noise_key = jax.random.fold_in(key, 11)
    channel_key = jax.random.fold_in(key, 12)
    offset_key = jax.random.fold_in(key, 13)
    shape = (IMAGES, height, width, C)
    noise = jnp.clip(jax.random.normal(noise_key, shape, jnp.float32), -4.0, 4.0)
    rise = math.log(3.0)
    channel_scale = jnp.exp(jax.random.uniform(channel_key, (C,), jnp.float32, math.log(0.3), math.log(3.0)))
    image_pos = jnp.arange(IMAGES, dtype=jnp.float32) / max(IMAGES - 1, 1)
    row_pos = jnp.arange(height, dtype=jnp.float32) / max(height - 1, 1)
    spatial_scale = jnp.exp(rise * (image_pos[:, None] + row_pos[None, :] - 1.0))
    offsets = 0.5 * jax.random.normal(offset_key, (IMAGES, 1, 1, C), jnp.float32)
    values = noise * spatial_scale[:, :, None, None] * channel_scale + offsets
    return jnp.clip(values, -40.0, 40.0).astype(jnp.bfloat16)


def draw_fine_level(key, part):
    return level_draw(key, HEIGHT, COLS)


def draw_middle_level(key, part):
    return level_draw(key, HEIGHT_MID, COLS_MID)


def draw_coarse_level(key, part):
    return level_draw(key, HEIGHT_TOP, COLS_TOP)


def gaussian(key, extent, scale, most, kind=jnp.bfloat16):
    entries = jax.random.normal(key, extent, jnp.float32) * scale
    return jnp.minimum(jnp.maximum(entries, -most), most).astype(kind)


def setup_inputs(seed: int = 0) -> dict:
    keys = jax.random.split(jax.random.key(seed), 10)
    return {
        "fine_level": draw_fine_level(jax.random.fold_in(keys[9], 71), 0),
        "middle_level": draw_middle_level(jax.random.fold_in(keys[9], 71), 0),
        "coarse_level": draw_coarse_level(jax.random.fold_in(keys[9], 71), 0),
        "two_input_weights": jnp.clip(jnp.exp(jax.random.uniform(keys[3], (LAYERS, 3, 2), jnp.float32, math.log(0.5), math.log(2.0))), 0.5, 2.0),
        "three_input_weights": jnp.clip(jnp.exp(jax.random.uniform(keys[4], (LAYERS, 3), jnp.float32, math.log(0.5), math.log(2.0))), 0.5, 2.0),
        "depthwise": gaussian(keys[5], (LAYERS, 4, 3, 3, C), 9 ** -0.5, 2.0),
        "pointwise": gaussian(keys[6], (LAYERS, 4, C, C), C ** -0.5, 0.3125),
        "bn_gain": jnp.clip(1.0 + 0.1 * jax.random.normal(keys[7], (LAYERS, 4, C), jnp.float32), 0.5, 1.5),
        "bn_bias": gaussian(keys[8], (LAYERS, 4, C), 0.5, 3.0, jnp.float32),
    }


def upsample(feature_maps):
    return jnp.repeat(jnp.repeat(feature_maps, 2, axis=1), 2, axis=2)

def reduce_resolution(feature_maps):
    lowest = jnp.array(-jnp.inf, feature_maps.dtype)
    padded = jnp.pad(feature_maps, ((0, 0), (0, 1), (0, 1), (0, 0)), constant_values=lowest)
    return lax.reduce_window(padded, lowest, lax.max, (1, 3, 3, 1), (1, 2, 2, 1), 'VALID')

def weighted_join_activate(inputs_list, weights):
    weight_sum = jnp.sum(weights) + 0.0001
    running = weights[0] * inputs_list[0].astype(jnp.float32)
    for position in range(1, len(inputs_list)):
        running = running + weights[position] * inputs_list[position].astype(jnp.float32)
    return jax.nn.silu(running / weight_sum).astype(jnp.bfloat16)

def separable(extended, kernel, projection):
    padded = jnp.pad(extended, ((0, 0), (0, 0), (1, 1), (0, 0)))
    height = extended.shape[1] - 2
    width = extended.shape[2]
    running = jnp.zeros((extended.shape[0], height, width, extended.shape[3]), jnp.float32)
    for row_tap in range(3):
        for col_tap in range(3):
            window = padded[:, row_tap:row_tap + height, col_tap:col_tap + width, :]
            running = running + window.astype(jnp.float32) * kernel[row_tap, col_tap].astype(jnp.float32)
    spatial = running.astype(jnp.bfloat16)
    projected = jnp.dot(spatial.reshape(-1, spatial.shape[-1]), projection, preferred_element_type=jnp.float32)
    return projected.reshape(spatial.shape)

def normalize(projected, gain, offset):
    center = lax.optimization_barrier(jnp.mean(projected, axis=(0, 1, 2)))
    centered = projected - center
    spread = lax.optimization_barrier(jnp.mean(centered * centered, axis=(0, 1, 2)))
    return (centered * lax.rsqrt(spread + 1e-05) * gain + offset).astype(jnp.bfloat16)

def node(activated, kernel, projection, gain, offset):
    padded = jnp.pad(activated, ((0, 0), (1, 1), (0, 0), (0, 0)))

    def one_image(image):
        return separable(image[None], kernel, projection)[0]
    projected = lax.map(one_image, padded)
    return normalize(projected, gain, offset)

def reference(fine_level, middle_level, coarse_level, two_input_weights, three_input_weights, depthwise, pointwise, bn_gain, bn_bias):
    fine, middle_grid, coarse_grid = (fine_level, middle_level, coarse_level)
    for bidirectional_layer in range(LAYERS):

        def run_layer_pair(index, activated):
            return node(activated, depthwise[bidirectional_layer, index], pointwise[bidirectional_layer, index], bn_gain[bidirectional_layer, index], bn_bias[bidirectional_layer, index])
        downward_middle = run_layer_pair(0, weighted_join_activate([middle_grid, upsample(coarse_grid)], two_input_weights[bidirectional_layer, 0]))
        updated_fine = run_layer_pair(1, weighted_join_activate([fine, upsample(downward_middle)], two_input_weights[bidirectional_layer, 1]))
        updated_middle = run_layer_pair(2, weighted_join_activate([middle_grid, downward_middle, reduce_resolution(updated_fine)], three_input_weights[bidirectional_layer]))
        updated_coarse = run_layer_pair(3, weighted_join_activate([coarse_grid, reduce_resolution(updated_middle)], two_input_weights[bidirectional_layer, 2]))
        fine, middle_grid, coarse_grid = (updated_fine, updated_middle, updated_coarse)
    return (fine, middle_grid, coarse_grid)
```

```python
import functools

import jax
import jax.numpy as jnp
from jax import lax
from jax.experimental import pallas as pl
from jax.experimental.pallas import tpu as pltpu
from jax.sharding import Mesh
from jax.sharding import PartitionSpec as P

LAYERS = 2
BATCH = ("batch_0", "batch_1", "batch_2")
MESH_ID = pl.DeviceIdType.MESH
HUB = 1
C = 384
K = 48
LOW = -1e30
EPS = 1e-05
F32 = jnp.float32
BF16 = jnp.bfloat16


def ring_distance(d, n):
    return min(d, n - d)


Z_OFFSETS = sorted(range(1, 8), key=lambda d: -ring_distance(d, 8))
XY_OFFSETS = sorted(
    [(a, b) for a in range(4) for b in range(4) if (a, b) != (0, 0)],
    key=lambda o: -(ring_distance(o[0], 4) + ring_distance(o[1], 4)),
)


def tiles(x):
    return x.reshape(x.shape[0] // 8, 8, x.shape[1])


def flat(x):
    return x.reshape(x.shape[0] * x.shape[1], x.shape[2])


def shifted_down(x):
    rolled = pltpu.roll(x, 1, axis=0)
    return jnp.where(lax.broadcasted_iota(jnp.int32, x.shape, 0) == 0, 0.0, rolled)


def shifted_up(x, fill):
    rolled = pltpu.roll(x, x.shape[0] - 1, axis=0)
    at_end = lax.broadcasted_iota(jnp.int32, x.shape, 0) == x.shape[0] - 1
    return jnp.where(at_end, fill, rolled)


def silu_of_double(h):
    return h + h * jnp.tanh(h)


def wait_bytes(ref, sem):
    pltpu.make_async_copy(ref, ref, sem).wait()


def kernel(
    counts,
    fine_hbm,
    mid_hbm,
    top_hbm,
    w2,
    w3,
    dw_hbm,
    pw_hbm,
    gain_hbm,
    bias_hbm,
    fine_out,
    mid_out,
    top_out,
    fine_nat,
    mid_nat,
    top_nat,
    dw_in,
    pw,
    gain,
    bias,
    dwb,
    perm_f,
    perm_m,
    back_f,
    back_m,
    base_f,
    act_f,
    mid_in,
    base_m,
    act_m,
    top_in,
    base_t,
    act_t,
    lifted,
    raw_m,
    raw_f,
    raw_t,
    col_f,
    col_m,
    pool_m,
    pool_t,
    spat,
    norm,
    halo_m,
    send_m,
    halo_p,
    send_p,
    halo_f,
    send_f,
    halo_q,
    send_q,
    halo_t,
    send_t,
    halo_c,
    send_c,
    ring,
    plane,
    fine_res,
    mid_res,
    top_res,
    in_sem,
    out_sem,
    ring_s,
    ring_r,
    plane_s,
    plane_r,
    halo_s,
    halo_r,
):
    y, x = lax.axis_index("batch_0"), lax.axis_index("batch_1")
    core, z = lax.axis_index("batch_2"), lax.axis_index("rows")
    in_ring = core * 8 + z
    in_plane = y * 4 + x
    is_hub = core == HUB
    has_above, has_below = z > 0, z < 7

    barrier = pltpu.get_barrier_semaphore()

    def greet(**device):
        pl.semaphore_signal(barrier, inc=1, device_id=device, device_id_type=MESH_ID)

    for d in range(8):
        for c in range(2):
            if d:
                greet(batch_2=lax.rem(core + c, 2), rows=lax.rem(z + d, 8))
    for a in range(4):
        for b in range(4):
            for c in range(2):
                if (a, b, c) != (0, 0, 0):
                    greet(
                        batch_0=lax.rem(y + a, 4),
                        batch_1=lax.rem(x + b, 4),
                        batch_2=lax.rem(core + c, 2),
                    )

    loads = {
        "top": pltpu.make_async_copy(top_hbm.at[0], top_nat.at[pl.ds(1, 2)], in_sem.at[0]),
        "mid": pltpu.make_async_copy(mid_hbm.at[0], mid_nat.at[pl.ds(1, 4)], in_sem.at[1]),
        "dw": pltpu.make_async_copy(dw_hbm, dw_in, in_sem.at[2]),
        "fine": pltpu.make_async_copy(fine_hbm.at[0], fine_nat.at[pl.ds(1, 8)], in_sem.at[3]),
        "pw": pltpu.make_async_copy(pw_hbm, pw, in_sem.at[4]),
        "gain": pltpu.make_async_copy(gain_hbm, gain, in_sem.at[5]),
        "bias": pltpu.make_async_copy(bias_hbm, bias, in_sem.at[6]),
    }
    for load in loads.values():
        load.start()

    def permutation(ref, back, parts):
        n = parts * K
        row = lax.broadcasted_iota(jnp.int32, (n, n), 0)
        col = lax.broadcasted_iota(jnp.int32, (n, n), 1)
        ref[...] = jnp.where(lax.rem(row, K) * parts + lax.div(row, K) == col, 1.0, 0.0).astype(BF16)
        back[...] = jnp.where(lax.rem(col, K) * parts + lax.div(col, K) == row, 1.0, 0.0).astype(
            BF16
        )

    permutation(perm_m, back_m, 2)
    permutation(perm_f, back_f, 4)

    def zeroed(ref):
        ref[...] = jnp.zeros(ref.shape, ref.dtype)

    @pl.when(z == 0)
    def _():
        for ref in (fine_nat.at[0], mid_nat.at[0], top_nat.at[0]):
            zeroed(ref)
        for l in range(LAYERS):
            for ref in (halo_m.at[l, 0], halo_p.at[l, 0], halo_q.at[l, 0]):
                zeroed(ref)
        for ref in (halo_f.at[0], halo_t.at[0], halo_c.at[0]):
            zeroed(ref)
        for node in range(8):
            zeroed(norm.at[node, 3])

    @pl.when(z == 7)
    def _():
        for ref in (fine_nat.at[9], mid_nat.at[5], top_nat.at[3]):
            zeroed(ref)
        for l in range(LAYERS):
            zeroed(halo_m.at[l, 1])
            for s in (1, 2):
                for ref in (halo_p.at[l, s], halo_q.at[l, s]):
                    ref[...] = jnp.full(ref.shape, LOW, BF16)
        for ref in (halo_f.at[1], halo_t.at[1], halo_c.at[1]):
            zeroed(ref)
        for node in range(8):
            zeroed(norm.at[node, 4])

    loads["dw"].wait()
    for l in range(LAYERS):
        for n in range(4):
            for i in range(3):
                taps = dw_in[l, n, i].astype(F32)
                for j in range(3):
                    dwb[l * 4 + n, 3 * i + j] = jnp.broadcast_to(taps[j : j + 1], (8, C))

    pl.semaphore_wait(barrier, 14 + 31)

    above = {"rows": jnp.maximum(z - 1, 0)}
    below = {"rows": jnp.minimum(z + 1, 7)}

    def to_above(src, dst, slot):
        return pltpu.make_async_remote_copy(
            src, dst, halo_s.at[slot], halo_r.at[slot], device_id=above, device_id_type=MESH_ID
        )

    def to_below(src, dst, slot):
        return pltpu.make_async_remote_copy(
            src, dst, halo_s.at[slot], halo_r.at[slot], device_id=below, device_id_type=MESH_ID
        )

    sends_up, sends_down = [], []

    def send(up, down):
        @pl.when(has_above)
        def _():
            for one in up:
                to_above(*one).start()

        @pl.when(has_below)
        def _():
            for one in down:
                to_below(*one).start()

        sends_up.extend(up)
        sends_down.extend(down)

    def receive(from_below, from_above):
        @pl.when(has_below)
        def _():
            for _, dst, slot in from_below:
                wait_bytes(dst, halo_r.at[slot])

        @pl.when(has_above)
        def _():
            for _, dst, slot in from_above:
                wait_bytes(dst, halo_r.at[slot])

    loads["top"].wait()
    loads["mid"].wait()
    first_up = [
        (mid_nat.at[1], mid_nat.at[5], 0),
        (top_nat.at[1], top_nat.at[3], 1),
    ]
    first_down = [
        (mid_nat.at[4], mid_nat.at[0], 2),
        (top_nat.at[2], top_nat.at[0], 3),
    ]
    send(first_up, first_down)
    loads["fine"].wait()
    fine_up = [(fine_nat.at[1], fine_nat.at[9], 4)]
    fine_down = [(fine_nat.at[8], fine_nat.at[0], 5)]
    send(fine_up, fine_down)

    def halves(weights):
        spread = [jnp.full((8, C), 1.0, F32) * w for w in weights]
        acc = spread[0]
        for one in spread[1:]:
            acc = acc + one
        acc = acc + 0.0001
        return [0.5 * one / acc for one in spread]

    def two(l, n):
        return halves([w2[l, n, 0], w2[l, n, 1]])

    def three(l):
        return halves([w3[l, 0], w3[l, 1], w3[l, 2]])

    def convolve(act, raw, index, height, planes, step_rows):
        lanes = planes * K

        def step(s, carry):
            total, squares = carry
            for dr in range(step_rows):
                r = s * step_rows + dr
                for c in range(3):
                    cs = pl.ds(c * 128, 128)
                    taps = [dwb[index, t, :, cs] for t in range(9)]
                    sums = []
                    for q in range(planes):
                        rows = [tiles(act[r + i, q, :, cs]) for i in range(3)]
                        sums.append(
                            [
                                flat(
                                    rows[0] * taps[j] + rows[1] * taps[3 + j] + rows[2] * taps[6 + j]
                                )
                                for j in range(3)
                            ]
                        )
                    for q in range(planes):
                        left = sums[q - 1][0] if q else shifted_down(sums[planes - 1][0])
                        right = sums[q + 1][2] if q + 1 < planes else shifted_up(sums[0][2], 0.0)
                        spat[pl.ds(dr * lanes + q * K, K), cs] = (left + sums[q][1] + right).astype(
                            BF16
                        )
            out = jnp.dot(
                spat[pl.ds(0, step_rows * lanes), :],
                pw[index // 4, index % 4],
                preferred_element_type=F32,
            )
            for dr in range(step_rows):
                for q in range(planes):
                    at = dr * lanes + q * K
                    raw[s * step_rows + dr, q] = out[at : at + K]
            out = tiles(out)
            return total + jnp.sum(out, axis=0), squares + jnp.sum(out * out, axis=0)

        start = (jnp.zeros((8, C), F32), jnp.zeros((8, C), F32))
        return lax.fori_loop(0, height // step_rows, step, start)

    def reduce_start(index, stats, local_count):
        total, squares = stats
        total = jnp.sum(total, axis=0, keepdims=True)
        squares = jnp.sum(squares, axis=0, keepdims=True)
        for c in range(3):
            ring[index, in_ring, c : c + 1, :] = total[:, c * 128 : (c + 1) * 128]
            ring[index, in_ring, 3 + c : 4 + c, :] = squares[:, c * 128 : (c + 1) * 128]
        norm[index, 2] = jnp.broadcast_to(total * (1.0 / local_count), (8, C))

        def to_hub(**device):
            pltpu.make_async_remote_copy(
                ring.at[index, in_ring],
                ring.at[index, in_ring],
                ring_s.at[index],
                ring_r.at[index],
                device_id=device,
                device_id_type=MESH_ID,
            ).start()

        @pl.when(jnp.logical_not(is_hub))
        def _():
            for d in Z_OFFSETS + [0]:
                to_hub(batch_2=HUB, rows=lax.rem(z + d, 8))

        @pl.when(is_hub)
        def _():
            for d in Z_OFFSETS:
                to_hub(rows=lax.rem(z + d, 8))
            wait_bytes(ring.at[index, pl.ds(0, 15)], ring_r.at[index])
            acc = ring[index, 0]
            for k in range(1, 16):
                acc = acc + ring[index, k]
            plane[index * 16 + in_plane] = acc

            def to_plane(**device):
                pltpu.make_async_remote_copy(
                    plane.at[index * 16 + in_plane],
                    plane.at[index * 16 + in_plane],
                    plane_s.at[index],
                    plane_r.at[index],
                    device_id=device,
                    device_id_type=MESH_ID,
                ).start()

            for a, b in XY_OFFSETS:
                at = {"batch_0": lax.rem(y + a, 4), "batch_1": lax.rem(x + b, 4)}
                to_plane(**at, batch_2=1 - HUB)
                to_plane(**at)
            to_plane(batch_2=1 - HUB)

    def reduce_end(index, count):
        @pl.when(is_hub)
        def _():
            wait_bytes(plane.at[pl.ds(index * 16, 15)], plane_r.at[index])

        @pl.when(jnp.logical_not(is_hub))
        def _():
            wait_bytes(plane.at[pl.ds(index * 16, 16)], plane_r.at[index])

        acc = plane[index * 16]
        for k in range(1, 16):
            acc = acc + plane[index * 16 + k]
        acc = acc * (1.0 / count)
        l, n = index // 4, index % 4
        for c in range(3):
            cs = pl.ds(c * 128, 128)
            center = acc[c : c + 1]
            spread = acc[3 + c : 4 + c] - center * center
            scale = gain[l, n : n + 1, cs] * lax.rsqrt(spread + EPS)
            shift = bias[l, n : n + 1, cs] - center * scale
            norm[index, 0, :, cs] = jnp.broadcast_to(scale, (8, 128))
            norm[index, 1, :, cs] = jnp.broadcast_to(shift, (8, 128))

    def centred(value, index):
        return flat(tiles(value) - norm[index, 2]).astype(BF16)

    def mean_up(index):
        return (norm.at[index, 2], norm.at[index, 4], 8 + 2 * index)

    def mean_down(index):
        return (norm.at[index, 2], norm.at[index, 3], 9 + 2 * index)

    def scale_shift(index, weight):
        scale, shift = norm[index, 0], norm[index, 1]
        if weight is not None:
            scale, shift = scale * weight, shift * weight
        shift_above = norm[index, 3] * scale + shift
        shift_below = norm[index, 4] * scale + shift
        return scale, shift, shift_above, shift_below

    def affine(value, scale, shift):
        return flat(tiles(value.astype(F32)) * scale + shift)

    def masked_edges(act, last):
        @pl.when(z == 0)
        def _():
            zeroed(act.at[0])

        @pl.when(z == 7)
        def _():
            zeroed(act.at[last])

    def each(n, fn):
        def step(i, _):
            fn(i)
            return 0

        lax.fori_loop(0, n, step, 0)

    def column_pool(load, planes):
        out = []
        for p in range(max(planes // 2, 1)):
            x0, x1 = load(2 * p), load(2 * p + 1)
            x2 = load(2 * p + 2) if 2 * p + 2 < planes else shifted_up(load(0), LOW)
            out.append(jnp.maximum(jnp.maximum(x0, x1), x2))
        return out

    mid_pair = range(2)

    for l in range(LAYERS):
        i0, i1, i2, i3 = (4 * l + n for n in range(4))
        mids = raw_m.at[2 * l]
        fines = raw_f.at[l]
        nexts = raw_m.at[2 * l + 1]
        tops = raw_t.at[l]

        own, up = two(l, 0)
        if l == 0:
            receive(first_up, first_down)

            def place_mid(e):
                out = jnp.dot(perm_m[...], mid_nat[e], preferred_element_type=F32)
                for p in mid_pair:
                    mid_in[e, p] = out[p * K : (p + 1) * K]

            each(6, place_mid)
            for e in range(4):
                top_in[e] = top_nat[e].astype(F32)
            loads["pw"].wait()
            loads["gain"].wait()
            loads["bias"].wait()
        else:
            scale, shift, shift_above, shift_below = scale_shift(3, None)
            for e in range(4):
                if e == 0:
                    top_in[e] = affine(halo_c[0], scale, shift_above)
                elif e == 3:
                    top_in[e] = affine(halo_c[1], scale, shift_below)
                else:
                    top_in[e] = affine(raw_t[0, e - 1, 0], scale, shift)

        def join_0(e):
            t = tiles(top_in[lax.div(e + 1, 2)]) * up
            for p in mid_pair:
                act_m[e, p] = flat(silu_of_double(tiles(mid_in[e, p]) * own + t))

        each(6, join_0)
        masked_edges(act_m, 5)
        stats = convolve(act_m, mids, i0, 4, 2, 2)
        reduce_start(i0, stats, 4 * 96)
        for p in mid_pair:
            send_m[l, 0, p] = centred(mids[0, p], i0)
            send_m[l, 1, p] = centred(mids[3, p], i0)
        up_0 = [(send_m.at[l, 0], halo_m.at[l, 1], 24 + 2 * l), mean_up(i0)]
        down_0 = [(send_m.at[l, 1], halo_m.at[l, 0], 25 + 2 * l), mean_down(i0)]
        send(up_0, down_0)

        own, up = two(l, 1)
        if l == 0:
            receive(fine_up, fine_down)

            def place_fine(e):
                out = jnp.dot(perm_f[...], fine_nat[e], preferred_element_type=F32)
                for q in range(4):
                    base_f[e, q] = flat(tiles(out[q * K : (q + 1) * K]) * own)

            each(10, place_fine)
        else:
            scale, shift, shift_above, shift_below = scale_shift(1, own)

            def place_fine(e):
                for q in range(4):
                    base_f[e + 1, q] = affine(raw_f[0, e, q], scale, shift)

            each(8, place_fine)
            for q in range(4):
                base_f[0, q] = affine(halo_f[0, q], scale, shift_above)
                base_f[9, q] = affine(halo_f[1, q], scale, shift_below)

        receive(up_0, down_0)
        reduce_end(i0, counts[1])

        scale, shift, shift_above, shift_below = scale_shift(i0, up)
        for p in mid_pair:
            lifted[0, p] = affine(halo_m[l, 0, p], scale, shift_above)
            lifted[5, p] = affine(halo_m[l, 1, p], scale, shift_below)

        def lift(e):
            for p in mid_pair:
                lifted[e + 1, p] = affine(mids[e, p], scale, shift)

        each(4, lift)

        def join_1(e):
            m = lax.div(e + 1, 2)
            for p in mid_pair:
                t = lifted[m, p]
                for q in (2 * p, 2 * p + 1):
                    act_f[e, q] = silu_of_double(base_f[e, q] + t)

        each(10, join_1)
        masked_edges(act_f, 9)
        stats = convolve(act_f, fines, i1, 8, 4, 1)
        reduce_start(i1, stats, 8 * 192)

        def pool_columns(r):
            for p, out in enumerate(column_pool(lambda q: fines[r, q], 4)):
                col_f[r, p] = out

        each(8, pool_columns)
        for p in mid_pair:
            first = jnp.maximum(jnp.maximum(col_f[0, p], col_f[1, p]), col_f[2, p])
            pool_m[1, p] = first
            send_p[l, 0, p] = centred(col_f[0, p], i1)
            send_p[l, 1, p] = centred(first, i1)
            send_p[l, 2, p] = centred(jnp.maximum(col_f[6, p], col_f[7, p]), i1)
        up_1 = [(send_p.at[l, pl.ds(0, 2)], halo_p.at[l, pl.ds(1, 2)], 28 + 2 * l), mean_up(i1)]
        down_1 = [(send_p.at[l, 2], halo_p.at[l, 0], 29 + 2 * l), mean_down(i1)]
        send(up_1, down_1)
        if l == 0:
            for q in range(4):
                send_f[0, q] = centred(fines[0, q], i1)
                send_f[1, q] = centred(fines[7, q], i1)
            up_f = [(send_f.at[0], halo_f.at[1], 32)]
            down_f = [(send_f.at[1], halo_f.at[0], 33)]
            send(up_f, down_f)

        w_mid, w_down, w_pool = three(l)
        scale, shift, shift_above, shift_below = scale_shift(i0, w_down)

        def known(e, value, one_shift):
            for p in mid_pair:
                base_m[e, p] = flat(
                    tiles(mid_in[e, p]) * w_mid + tiles(value(p).astype(F32)) * scale + one_shift
                )

        known(0, lambda p: halo_m[l, 0, p], shift_above)
        known(5, lambda p: halo_m[l, 1, p], shift_below)
        each(4, lambda e: known(e + 1, lambda p: mids[e, p], shift))
        w_top, w_up = two(l, 2)
        for e in range(4):
            base_t[e] = flat(tiles(top_in[e]) * w_top)
        for i in (1, 2):
            for p in mid_pair:
                pool_m[i + 1, p] = jnp.maximum(
                    jnp.maximum(col_f[2 * i, p], col_f[2 * i + 1, p]), col_f[2 * i + 2, p]
                )
        receive(up_1, down_1)
        mean_above, mean_below = norm[i1, 3], norm[i1, 4]
        for p in mid_pair:
            pool_m[0, p] = jnp.maximum(
                flat(tiles(halo_p[l, 0, p].astype(F32)) + mean_above), col_f[0, p]
            )
            pool_m[4, p] = jnp.maximum(
                jnp.maximum(col_f[6, p], col_f[7, p]),
                flat(tiles(halo_p[l, 1, p].astype(F32)) + mean_below),
            )
            pool_m[5, p] = flat(tiles(halo_p[l, 2, p].astype(F32)) + mean_below)
        reduce_end(i1, counts[0])

        scale, shift, _, _ = scale_shift(i1, w_pool)

        def join_2(e):
            for p in mid_pair:
                act_m[e, p] = flat(
                    silu_of_double(tiles(base_m[e, p]) + (tiles(pool_m[e, p]) * scale + shift))
                )

        each(6, join_2)
        masked_edges(act_m, 5)
        stats = convolve(act_m, nexts, i2, 4, 2, 2)
        reduce_start(i2, stats, 4 * 96)
        for r in range(4):
            col_m[r] = column_pool(lambda q: nexts[r, q], 2)[0]
        first = jnp.maximum(jnp.maximum(col_m[0], col_m[1]), col_m[2])
        pool_t[1] = first
        send_q[l, 0] = centred(col_m[0], i2)
        send_q[l, 1] = centred(first, i2)
        send_q[l, 2] = centred(jnp.maximum(col_m[2], col_m[3]), i2)
        up_2 = [(send_q.at[l, pl.ds(0, 2)], halo_q.at[l, pl.ds(1, 2)], 34 + 2 * l), mean_up(i2)]
        down_2 = [(send_q.at[l, 2], halo_q.at[l, 0], 35 + 2 * l), mean_down(i2)]
        send(up_2, down_2)
        if l == 0:
            for p in mid_pair:
                send_t[0, p] = centred(nexts[0, p], i2)
                send_t[1, p] = centred(nexts[3, p], i2)
            up_t = [(send_t.at[0], halo_t.at[1], 38)]
            down_t = [(send_t.at[1], halo_t.at[0], 39)]
            send(up_t, down_t)
            receive(up_f, down_f)
        else:
            scale, shift, _, _ = scale_shift(i1, None)

            def finish_fine(r):
                for q in range(4):
                    spat[pl.ds(q * K, K), :] = affine(fines[r, q], scale, shift).astype(BF16)
                fine_res[r] = jnp.dot(
                    back_f[...], spat[pl.ds(0, 4 * K), :], preferred_element_type=F32
                ).astype(BF16)

            each(8, finish_fine)
            fine_store = pltpu.make_async_copy(fine_res, fine_out.at[0], out_sem.at[0])
            fine_store.start()
        receive(up_2, down_2)
        mean_above, mean_below = norm[i2, 3], norm[i2, 4]
        pool_t[0] = jnp.maximum(flat(tiles(halo_q[l, 0].astype(F32)) + mean_above), col_m[0])
        pool_t[2] = jnp.maximum(
            jnp.maximum(col_m[2], col_m[3]), flat(tiles(halo_q[l, 1].astype(F32)) + mean_below)
        )
        pool_t[3] = flat(tiles(halo_q[l, 2].astype(F32)) + mean_below)
        reduce_end(i2, counts[1])

        scale, shift, _, _ = scale_shift(i2, w_up)
        for e in range(4):
            act_t[e, 0] = flat(
                silu_of_double(tiles(base_t[e]) + (tiles(pool_t[e]) * scale + shift))
            )
        masked_edges(act_t, 3)
        stats = convolve(act_t, tops, i3, 2, 1, 2)
        reduce_start(i3, stats, 2 * 48)
        scale, shift, shift_above, shift_below = scale_shift(i2, None)
        if l == 0:
            send_c[0] = centred(tops[0, 0], i3)
            send_c[1] = centred(tops[1, 0], i3)
            up_3 = [(send_c.at[0], halo_c.at[1], 40), mean_up(i3)]
            down_3 = [(send_c.at[1], halo_c.at[0], 41), mean_down(i3)]
            send(up_3, down_3)
            receive(up_t, down_t)
            for p in mid_pair:
                mid_in[0, p] = affine(halo_t[0, p], scale, shift_above)
                mid_in[5, p] = affine(halo_t[1, p], scale, shift_below)

            def normalize_mid(e):
                for p in mid_pair:
                    mid_in[e + 1, p] = affine(nexts[e, p], scale, shift)

            each(4, normalize_mid)
            receive(up_3, down_3)
            reduce_end(i3, counts[2])
        else:

            def finish_mid(r):
                for p in mid_pair:
                    spat[pl.ds(p * K, K), :] = affine(nexts[r, p], scale, shift).astype(BF16)
                mid_res[r] = jnp.dot(
                    back_m[...], spat[pl.ds(0, 2 * K), :], preferred_element_type=F32
                ).astype(BF16)

            each(4, finish_mid)
            mid_store = pltpu.make_async_copy(mid_res, mid_out.at[0], out_sem.at[1])
            mid_store.start()
            reduce_end(i3, counts[2])
            scale, shift, _, _ = scale_shift(i3, None)
            for e in range(2):
                top_res[e] = affine(tops[e, 0], scale, shift).astype(BF16)
            top_store = pltpu.make_async_copy(top_res, top_out.at[0], out_sem.at[2])
            top_store.start()

    @pl.when(has_above)
    def _():
        for src, _, slot in sends_up:
            wait_bytes(src, halo_s.at[slot])

    @pl.when(has_below)
    def _():
        for src, _, slot in sends_down:
            wait_bytes(src, halo_s.at[slot])

    @pl.when(jnp.logical_not(is_hub))
    def _():
        for index in range(8):
            wait_bytes(ring.at[index, pl.ds(0, 8)], ring_s.at[index])

    @pl.when(is_hub)
    def _():
        for index in range(8):
            wait_bytes(ring.at[index, pl.ds(0, 7)], ring_s.at[index])
            wait_bytes(plane.at[pl.ds(0, 31)], plane_s.at[index])
    fine_store.wait()
    mid_store.wait()
    top_store.wait()


def body(
    fine_level,
    middle_level,
    coarse_level,
    two_input_weights,
    three_input_weights,
    depthwise,
    pointwise,
    bn_gain,
    bn_bias,
):
    devices = lax.axis_size(BATCH) * lax.axis_size("rows")
    counts = tuple(
        float(a.shape[0] * a.shape[1] * a.shape[2] * devices)
        for a in (fine_level, middle_level, coarse_level)
    )
    any_space = pl.BlockSpec(memory_space=pl.ANY)
    smem = pl.BlockSpec(memory_space=pltpu.SMEM)
    vmem = pltpu.VMEM
    dma = pltpu.SemaphoreType.DMA
    scratch = [
        vmem((10, 192, C), BF16),
        vmem((6, 96, C), BF16),
        vmem((4, 48, C), BF16),
        vmem((2, 4, 3, 3, C), BF16),
        vmem((2, 4, C, C), BF16),
        vmem((2, 4, C), F32),
        vmem((2, 4, C), F32),
        vmem((8, 9, 8, C), F32),
        vmem((192, 192), BF16),
        vmem((96, 96), BF16),
        vmem((192, 192), BF16),
        vmem((96, 96), BF16),
        vmem((10, 4, K, C), F32),
        vmem((10, 4, K, C), F32),
        vmem((6, 2, K, C), F32),
        vmem((6, 2, K, C), F32),
        vmem((6, 2, K, C), F32),
        vmem((4, K, C), F32),
        vmem((4, K, C), F32),
        vmem((4, 1, K, C), F32),
        vmem((6, 2, K, C), F32),
        vmem((4, 4, 2, K, C), F32),
        vmem((2, 8, 4, K, C), F32),
        vmem((2, 2, 1, K, C), F32),
        vmem((8, 2, K, C), F32),
        vmem((4, K, C), F32),
        vmem((6, 2, K, C), F32),
        vmem((4, K, C), F32),
        vmem((2 * 96, C), BF16),
        vmem((8, 5, 8, C), F32),
        vmem((2, 2, 2, K, C), BF16),
        vmem((2, 2, 2, K, C), BF16),
        vmem((2, 3, 2, K, C), BF16),
        vmem((2, 3, 2, K, C), BF16),
        vmem((2, 4, K, C), BF16),
        vmem((2, 4, K, C), BF16),
        vmem((2, 3, K, C), BF16),
        vmem((2, 3, K, C), BF16),
        vmem((2, 2, K, C), BF16),
        vmem((2, 2, K, C), BF16),
        vmem((2, K, C), BF16),
        vmem((2, K, C), BF16),
        vmem((8, 16, 8, 128), F32),
        vmem((8 * 16, 8, 128), F32),
        vmem((8, 192, C), BF16),
        vmem((4, 96, C), BF16),
        vmem((2, 48, C), BF16),
        dma((7,)),
        dma((3,)),
        dma((8,)),
        dma((8,)),
        dma((8,)),
        dma((8,)),
        dma((42,)),
        dma((42,)),
    ]
    return pl.pallas_call(
        functools.partial(kernel, counts),
        out_shape=tuple(
            jax.ShapeDtypeStruct(a.shape, BF16) for a in (fine_level, middle_level, coarse_level)
        ),
        in_specs=[any_space] * 3 + [smem] * 2 + [any_space] * 4,
        out_specs=(any_space,) * 3,
        scratch_shapes=scratch,
        name="bifpn",
        compiler_params=pltpu.CompilerParams(
            collective_id=0, has_side_effects=True, vmem_limit_bytes=60 * 1024 * 1024
        ),
    )(
        fine_level,
        middle_level,
        coarse_level,
        two_input_weights,
        three_input_weights,
        depthwise,
        pointwise,
        bn_gain,
        bn_bias,
    )


def solution(mesh):
    split = Mesh(
        mesh.devices.reshape(4, 4, 2, mesh.shape["rows"]), ("batch_0", "batch_1", "batch_2", "rows")
    )
    level = P(BATCH, "rows", None, None)
    return jax.shard_map(
        body,
        mesh=split,
        in_specs=(level,) * 3 + (P(),) * 6,
        out_specs=(level,) * 3,
        check_vma=False,
    )
```

```python
import functools

import jax
import jax.numpy as jnp
from jax import lax
from jax.experimental import pallas as pl
from jax.experimental.pallas import tpu as pltpu
from jax.sharding import Mesh
from jax.sharding import PartitionSpec as P

LAYERS = 2
BATCH = ("batch_0", "batch_1", "batch_2")
MESH_ID = pl.DeviceIdType.MESH
HUB = 1
C = 384
K = 48
LOW = -1e30
EPS = 1e-05
F32 = jnp.float32
BF16 = jnp.bfloat16


def ring_distance(d, n):
    return min(d, n - d)


Z_OFFSETS = sorted(range(1, 8), key=lambda d: -ring_distance(d, 8))
XY_OFFSETS = sorted(
    [(a, b) for a in range(4) for b in range(4) if (a, b) != (0, 0)],
    key=lambda o: -(ring_distance(o[0], 4) + ring_distance(o[1], 4)),
)


def tiles(x):
    return x.reshape(x.shape[0] // 8, 8, x.shape[1])


def flat(x):
    return x.reshape(x.shape[0] * x.shape[1], x.shape[2])


def shifted_down(x):
    rolled = pltpu.roll(x, 1, axis=0)
    return jnp.where(lax.broadcasted_iota(jnp.int32, x.shape, 0) == 0, 0.0, rolled)


def shifted_up(x, fill):
    rolled = pltpu.roll(x, x.shape[0] - 1, axis=0)
    at_end = lax.broadcasted_iota(jnp.int32, x.shape, 0) == x.shape[0] - 1
    return jnp.where(at_end, fill, rolled)


def silu_of_double(h):
    return h + h * jnp.tanh(h)


def wait_bytes(ref, sem):
    pltpu.make_async_copy(ref, ref, sem).wait()


def kernel(
    counts,
    fine_hbm,
    mid_hbm,
    top_hbm,
    w2,
    w3,
    dw_hbm,
    pw_hbm,
    gain_hbm,
    bias_hbm,
    fine_out,
    mid_out,
    top_out,
    fine_nat,
    mid_nat,
    top_nat,
    dw_in,
    pw,
    gain,
    bias,
    dwb,
    perm_f,
    perm_m,
    back_f,
    back_m,
    base_f,
    act_f,
    mid_in,
    base_m,
    act_m,
    top_in,
    base_t,
    act_t,
    lifted,
    raw_m,
    raw_f,
    raw_t,
    col_f,
    col_m,
    pool_m,
    pool_t,
    spat,
    norm,
    halo_m,
    send_m,
    halo_p,
    send_p,
    halo_f,
    send_f,
    halo_q,
    send_q,
    halo_t,
    send_t,
    halo_c,
    send_c,
    ring,
    plane,
    in_sem,
    ring_s,
    ring_r,
    plane_s,
    plane_r,
    halo_s,
    halo_r,
):
    y, x = lax.axis_index("batch_0"), lax.axis_index("batch_1")
    core, z = lax.axis_index("batch_2"), lax.axis_index("rows")
    in_plane = core * 16 + y * 4 + x
    is_hub = core == HUB
    has_above, has_below = z > 0, z < 7

    barrier = pltpu.get_barrier_semaphore()

    def greet(**device):
        pl.semaphore_signal(barrier, inc=1, device_id=device, device_id_type=MESH_ID)

    for d in range(8):
        for c in range(2):
            if d:
                greet(batch_2=lax.rem(core + c, 2), rows=lax.rem(z + d, 8))
    for a in range(4):
        for b in range(4):
            for c in range(2):
                if (a, b, c) != (0, 0, 0):
                    greet(
                        batch_0=lax.rem(y + a, 4),
                        batch_1=lax.rem(x + b, 4),
                        batch_2=lax.rem(core + c, 2),
                    )

    loads = {
        "top": pltpu.make_async_copy(top_hbm.at[0], top_nat.at[pl.ds(1, 2)], in_sem.at[0]),
        "mid": pltpu.make_async_copy(mid_hbm.at[0], mid_nat.at[pl.ds(1, 4)], in_sem.at[1]),
        "dw": pltpu.make_async_copy(dw_hbm, dw_in, in_sem.at[2]),
        "fine": pltpu.make_async_copy(fine_hbm.at[0], fine_nat.at[pl.ds(1, 8)], in_sem.at[3]),
        "pw": pltpu.make_async_copy(pw_hbm.at[0, 0], pw.at[0, 0], in_sem.at[4]),
        "pw_0": pltpu.make_async_copy(pw_hbm.at[0, pl.ds(1, 3)], pw.at[0, pl.ds(1, 3)], in_sem.at[7]),
        "pw_1": pltpu.make_async_copy(pw_hbm.at[1], pw.at[1], in_sem.at[8]),
        "gain": pltpu.make_async_copy(gain_hbm, gain, in_sem.at[5]),
        "bias": pltpu.make_async_copy(bias_hbm, bias, in_sem.at[6]),
    }
    for load in loads.values():
        load.start()

    def permutation(ref, back, parts):
        n = parts * K
        row = lax.broadcasted_iota(jnp.int32, (n, n), 0)
        col = lax.broadcasted_iota(jnp.int32, (n, n), 1)
        ref[...] = jnp.where(lax.rem(row, K) * parts + lax.div(row, K) == col, 1.0, 0.0).astype(BF16)
        back[...] = jnp.where(lax.rem(col, K) * parts + lax.div(col, K) == row, 1.0, 0.0).astype(
            BF16
        )

    permutation(perm_m, back_m, 2)
    permutation(perm_f, back_f, 4)

    def zeroed(ref):
        ref[...] = jnp.zeros(ref.shape, ref.dtype)

    @pl.when(z == 0)
    def _():
        for ref in (fine_nat.at[0], mid_nat.at[0], top_nat.at[0]):
            zeroed(ref)
        for l in range(LAYERS):
            for ref in (halo_m.at[l, 0], halo_p.at[l, 0], halo_q.at[l, 0]):
                zeroed(ref)
        for ref in (halo_f.at[0], halo_t.at[0], halo_c.at[0]):
            zeroed(ref)
        for node in range(8):
            zeroed(norm.at[node, 3])

    @pl.when(z == 7)
    def _():
        for ref in (fine_nat.at[9], mid_nat.at[5], top_nat.at[3]):
            zeroed(ref)
        for l in range(LAYERS):
            zeroed(halo_m.at[l, 1])
            for s in (1, 2):
                for ref in (halo_p.at[l, s], halo_q.at[l, s]):
                    ref[...] = jnp.full(ref.shape, LOW, BF16)
        for ref in (halo_f.at[1], halo_t.at[1], halo_c.at[1]):
            zeroed(ref)
        for node in range(8):
            zeroed(norm.at[node, 4])

    loads["dw"].wait()
    for l in range(LAYERS):
        for i in range(3):
            for j in range(3):
                taps = dw_in[l, i, j].astype(F32)
                for n in range(4):
                    dwb[l * 4 + n, 3 * i + j] = jnp.broadcast_to(taps[n : n + 1], (8, C))

    pl.semaphore_wait(barrier, 14 + 31)

    above = {"rows": jnp.maximum(z - 1, 0)}
    below = {"rows": jnp.minimum(z + 1, 7)}

    def to_above(src, dst, slot):
        return pltpu.make_async_remote_copy(
            src, dst, halo_s.at[slot], halo_r.at[slot], device_id=above, device_id_type=MESH_ID
        )

    def to_below(src, dst, slot):
        return pltpu.make_async_remote_copy(
            src, dst, halo_s.at[slot], halo_r.at[slot], device_id=below, device_id_type=MESH_ID
        )

    sends_up, sends_down = [], []

    def send(up, down):
        @pl.when(has_above)
        def _():
            for one in up:
                to_above(*one).start()

        @pl.when(has_below)
        def _():
            for one in down:
                to_below(*one).start()

        sends_up.extend(up)
        sends_down.extend(down)

    def receive(from_below, from_above):
        @pl.when(has_below)
        def _():
            for _, dst, slot in from_below:
                wait_bytes(dst, halo_r.at[slot])

        @pl.when(has_above)
        def _():
            for _, dst, slot in from_above:
                wait_bytes(dst, halo_r.at[slot])

    loads["top"].wait()
    loads["mid"].wait()
    first_up = [
        (mid_nat.at[1], mid_nat.at[5], 0),
        (top_nat.at[1], top_nat.at[3], 1),
    ]
    first_down = [
        (mid_nat.at[4], mid_nat.at[0], 2),
        (top_nat.at[2], top_nat.at[0], 3),
    ]
    send(first_up, first_down)
    loads["fine"].wait()
    fine_up = [(fine_nat.at[1], fine_nat.at[9], 4)]
    fine_down = [(fine_nat.at[8], fine_nat.at[0], 5)]
    send(fine_up, fine_down)

    def halves(weights):
        spread = [jnp.full((8, C), 1.0, F32) * w for w in weights]
        acc = spread[0]
        for one in spread[1:]:
            acc = acc + one
        acc = acc + 0.0001
        return [0.5 * one / acc for one in spread]

    def two(l, n):
        return halves([w2[l, 0, n], w2[l, 1, n]])

    def three(l):
        return halves([w3[l, 0], w3[l, 1], w3[l, 2]])

    def convolve(act, raw, index, height, planes, step_rows, dot_rows):
        lanes = planes * K

        def depthwise(r, at):
            for c in range(3):
                cs = pl.ds(c * 128, 128)
                taps = [dwb[index, t, :, cs] for t in range(9)]
                sums = []
                for q in range(planes):
                    rows = [tiles(act[r + i, q, :, cs]) for i in range(3)]
                    sums.append(
                        [
                            flat(rows[0] * taps[j] + rows[1] * taps[3 + j] + rows[2] * taps[6 + j])
                            for j in range(3)
                        ]
                    )
                for q in range(planes):
                    left = sums[q - 1][0] if q else shifted_down(sums[planes - 1][0])
                    right = sums[q + 1][2] if q + 1 < planes else shifted_up(sums[0][2], 0.0)
                    spat[pl.ds(at + q * K, K), cs] = (left + sums[q][1] + right).astype(BF16)

        def step(s, carry):
            total, squares = carry
            for first in range(0, step_rows, dot_rows):
                for dr in range(first, first + dot_rows):
                    depthwise(s * step_rows + dr, dr * lanes)
                out = jnp.dot(
                    spat[pl.ds(first * lanes, dot_rows * lanes), :],
                    pw[index // 4, index % 4],
                    preferred_element_type=F32,
                )
                for dr in range(dot_rows):
                    for q in range(planes):
                        at = dr * lanes + q * K
                        raw[s * step_rows + first + dr, q] = out[at : at + K]
                out = tiles(out)
                total, squares = total + jnp.sum(out, axis=0), squares + jnp.sum(out * out, axis=0)
            return total, squares

        start = (jnp.zeros((8, C), F32), jnp.zeros((8, C), F32))
        return lax.fori_loop(0, height // step_rows, step, start)

    def slots(buffer, first, n):
        return buffer.at[pl.ds(first, n), pl.ds(0, 6)]

    def push(buffer, slot, sent, received, **device):
        pltpu.make_async_remote_copy(
            buffer.at[slot, pl.ds(0, 6)],
            buffer.at[slot, pl.ds(0, 6)],
            sent,
            received,
            device_id=device,
            device_id_type=MESH_ID,
        ).start()

    def added(buffer, first, n):
        terms = [buffer[first + k, 0:6] for k in range(n)]
        while len(terms) > 1:
            terms = [terms[k] + terms[k + 1] for k in range(0, len(terms), 2)]
        return terms[0]

    def plane_device(a, b):
        return {"batch_0": lax.rem(y + a, 4), "batch_1": lax.rem(x + b, 4)}

    def reduce_start(index, stats, local_count):
        total, squares = stats
        total = jnp.sum(total, axis=0, keepdims=True)
        squares = jnp.sum(squares, axis=0, keepdims=True)
        mine = index * 32 + in_plane
        for c in range(3):
            plane[mine, c : c + 1, :] = total[:, c * 128 : (c + 1) * 128]
            plane[mine, 3 + c : 4 + c, :] = squares[:, c * 128 : (c + 1) * 128]
        norm[index, 2] = jnp.broadcast_to(total * (1.0 / local_count), (8, C))

        for a, b in XY_OFFSETS:
            push(
                plane, mine, plane_s.at[index], plane_r.at[index], **plane_device(a, b), batch_2=HUB
            )

        @pl.when(jnp.logical_not(is_hub))
        def _():
            push(plane, mine, plane_s.at[index], plane_r.at[index], batch_2=HUB)

    def reduce_middle(index):
        @pl.when(is_hub)
        def _():
            wait_bytes(slots(plane, index * 32, 31), plane_r.at[index])
            mine = index * 8 + z
            ring[mine, 0:6] = added(plane, index * 32, 32)
            for d in Z_OFFSETS:
                at = lax.rem(z + d, 8)
                push(ring, mine, ring_s.at[index], ring_r.at[index], batch_2=1 - HUB, rows=at)
                push(ring, mine, ring_s.at[index], ring_r.at[index], rows=at)
            push(ring, mine, ring_s.at[index], ring_r.at[index], batch_2=1 - HUB)

    def reduce_end(index, count):
        @pl.when(is_hub)
        def _():
            wait_bytes(slots(ring, index * 8, 7), ring_r.at[index])

        @pl.when(jnp.logical_not(is_hub))
        def _():
            wait_bytes(slots(ring, index * 8, 8), ring_r.at[index])

        acc = added(ring, index * 8, 8) * (1.0 / count)
        l, n = index // 4, index % 4
        for c in range(3):
            cs = pl.ds(c * 128, 128)
            center = acc[c : c + 1]
            spread = acc[3 + c : 4 + c] - center * center
            scale = gain[l, n : n + 1, cs] * lax.rsqrt(spread + EPS)
            shift = bias[l, n : n + 1, cs] - center * scale
            norm[index, 0, :, cs] = jnp.broadcast_to(scale, (8, 128))
            norm[index, 1, :, cs] = jnp.broadcast_to(shift, (8, 128))

    def centred(value, index):
        return flat(tiles(value) - norm[index, 2]).astype(BF16)

    def mean_up(index):
        return (norm.at[index, 2], norm.at[index, 4], 8 + 2 * index)

    def mean_down(index):
        return (norm.at[index, 2], norm.at[index, 3], 9 + 2 * index)

    def scale_shift(index, weight):
        scale, shift = norm[index, 0], norm[index, 1]
        if weight is not None:
            scale, shift = scale * weight, shift * weight
        shift_above = norm[index, 3] * scale + shift
        shift_below = norm[index, 4] * scale + shift
        return scale, shift, shift_above, shift_below

    def affine(value, scale, shift):
        return flat(tiles(value.astype(F32)) * scale + shift)

    def masked_edges(act, last):
        @pl.when(z == 0)
        def _():
            zeroed(act.at[0])

        @pl.when(z == 7)
        def _():
            zeroed(act.at[last])

    def each(n, fn):
        def step(i, _):
            fn(i)
            return 0

        lax.fori_loop(0, n, step, 0)

    def column_pool(load, planes):
        out = []
        for p in range(max(planes // 2, 1)):
            x0, x1 = load(2 * p), load(2 * p + 1)
            x2 = load(2 * p + 2) if 2 * p + 2 < planes else shifted_up(load(0), LOW)
            out.append(jnp.maximum(jnp.maximum(x0, x1), x2))
        return out

    mid_pair = range(2)

    for l in range(LAYERS):
        i0, i1, i2, i3 = (4 * l + n for n in range(4))
        mids = raw_m.at[2 * l]
        fines = raw_f.at[l]
        nexts = raw_m.at[2 * l + 1]
        tops = raw_t.at[l]

        own, up = two(l, 0)
        if l == 0:
            receive(first_up, first_down)

            def place_mid(e):
                out = jnp.dot(perm_m[...], mid_nat[e], preferred_element_type=F32)
                for p in mid_pair:
                    mid_in[e, p] = out[p * K : (p + 1) * K]

            each(6, place_mid)
            for e in range(4):
                top_in[e] = top_nat[e].astype(F32)
            loads["pw"].wait()
        else:
            scale, shift, shift_above, shift_below = scale_shift(3, None)
            for e in range(4):
                if e == 0:
                    top_in[e] = affine(halo_c[0], scale, shift_above)
                elif e == 3:
                    top_in[e] = affine(halo_c[1], scale, shift_below)
                else:
                    top_in[e] = affine(raw_t[0, e - 1, 0], scale, shift)

        def join_0(e):
            t = tiles(top_in[lax.div(e + 1, 2)]) * up
            for p in mid_pair:
                act_m[e, p] = flat(silu_of_double(tiles(mid_in[e, p]) * own + t))

        each(6, join_0)
        masked_edges(act_m, 5)
        stats = convolve(act_m, mids, i0, 4, 2, 4, 2)
        reduce_start(i0, stats, 4 * 96)
        for p in mid_pair:
            send_m[l, 0, p] = centred(mids[0, p], i0)
            send_m[l, 1, p] = centred(mids[3, p], i0)
        up_0 = [(send_m.at[l, 0], halo_m.at[l, 1], 24 + 2 * l), mean_up(i0)]
        down_0 = [(send_m.at[l, 1], halo_m.at[l, 0], 25 + 2 * l), mean_down(i0)]
        send(up_0, down_0)
        reduce_middle(i0)

        own, up = two(l, 1)
        if l == 0:
            receive(fine_up, fine_down)

            def place_fine(e):
                out = jnp.dot(perm_f[...], fine_nat[e], preferred_element_type=F32)
                for q in range(4):
                    base_f[e, q] = flat(tiles(out[q * K : (q + 1) * K]) * own)

            each(10, place_fine)
        else:
            receive(up_f, down_f)
            scale, shift, shift_above, shift_below = scale_shift(1, own)

            def place_fine(e):
                for q in range(4):
                    base_f[e + 1, q] = affine(raw_f[0, e, q], scale, shift)

            each(8, place_fine)
            for q in range(4):
                base_f[0, q] = affine(halo_f[0, q], scale, shift_above)
                base_f[9, q] = affine(halo_f[1, q], scale, shift_below)

        receive(up_0, down_0)
        if l == 0:
            for name in ("pw_0", "pw_1", "gain", "bias"):
                loads[name].wait()
        reduce_end(i0, counts[1])

        scale, shift, shift_above, shift_below = scale_shift(i0, up)
        for p in mid_pair:
            lifted[0, p] = affine(halo_m[l, 0, p], scale, shift_above)
            lifted[5, p] = affine(halo_m[l, 1, p], scale, shift_below)

        def lift(e):
            for p in mid_pair:
                lifted[e + 1, p] = affine(mids[e, p], scale, shift)

        each(4, lift)

        def join_1(e):
            m = lax.div(e + 1, 2)
            for p in mid_pair:
                t = lifted[m, p]
                for q in (2 * p, 2 * p + 1):
                    act_f[e, q] = silu_of_double(base_f[e, q] + t)

        each(10, join_1)
        masked_edges(act_f, 9)
        stats = convolve(act_f, fines, i1, 8, 4, 4, 1)
        reduce_start(i1, stats, 8 * 192)

        def pool_columns(r):
            for p, out in enumerate(column_pool(lambda q: fines[r, q], 4)):
                col_f[r, p] = out

        each(8, pool_columns)
        for p in mid_pair:
            first = jnp.maximum(jnp.maximum(col_f[0, p], col_f[1, p]), col_f[2, p])
            pool_m[1, p] = first
            send_p[l, 0, p] = centred(col_f[0, p], i1)
            send_p[l, 1, p] = centred(first, i1)
            send_p[l, 2, p] = centred(jnp.maximum(col_f[6, p], col_f[7, p]), i1)
        up_1 = [(send_p.at[l, pl.ds(0, 2)], halo_p.at[l, pl.ds(1, 2)], 28 + 2 * l), mean_up(i1)]
        down_1 = [(send_p.at[l, 2], halo_p.at[l, 0], 29 + 2 * l), mean_down(i1)]
        send(up_1, down_1)
        reduce_middle(i1)
        if l == 0:
            for q in range(4):
                send_f[0, q] = centred(fines[0, q], i1)
                send_f[1, q] = centred(fines[7, q], i1)

        w_mid, w_down, w_pool = three(l)
        scale, shift, shift_above, shift_below = scale_shift(i0, w_down)

        def known(e, value, one_shift):
            for p in mid_pair:
                base_m[e, p] = flat(
                    tiles(mid_in[e, p]) * w_mid + tiles(value(p).astype(F32)) * scale + one_shift
                )

        known(0, lambda p: halo_m[l, 0, p], shift_above)
        known(5, lambda p: halo_m[l, 1, p], shift_below)
        each(4, lambda e: known(e + 1, lambda p: mids[e, p], shift))
        w_top, w_up = two(l, 2)
        for e in range(4):
            base_t[e] = flat(tiles(top_in[e]) * w_top)
        for i in (1, 2):
            for p in mid_pair:
                pool_m[i + 1, p] = jnp.maximum(
                    jnp.maximum(col_f[2 * i, p], col_f[2 * i + 1, p]), col_f[2 * i + 2, p]
                )
        receive(up_1, down_1)
        mean_above, mean_below = norm[i1, 3], norm[i1, 4]
        for p in mid_pair:
            pool_m[0, p] = jnp.maximum(
                flat(tiles(halo_p[l, 0, p].astype(F32)) + mean_above), col_f[0, p]
            )
            pool_m[4, p] = jnp.maximum(
                jnp.maximum(col_f[6, p], col_f[7, p]),
                flat(tiles(halo_p[l, 1, p].astype(F32)) + mean_below),
            )
            pool_m[5, p] = flat(tiles(halo_p[l, 2, p].astype(F32)) + mean_below)
        reduce_end(i1, counts[0])

        scale, shift, _, _ = scale_shift(i1, w_pool)

        def join_2(e):
            for p in mid_pair:
                act_m[e, p] = flat(
                    silu_of_double(tiles(base_m[e, p]) + (tiles(pool_m[e, p]) * scale + shift))
                )

        each(6, join_2)
        masked_edges(act_m, 5)
        stats = convolve(act_m, nexts, i2, 4, 2, 4, 2)
        reduce_start(i2, stats, 4 * 96)
        for r in range(4):
            col_m[r] = column_pool(lambda q: nexts[r, q], 2)[0]
        first = jnp.maximum(jnp.maximum(col_m[0], col_m[1]), col_m[2])
        pool_t[1] = first
        send_q[l, 0] = centred(col_m[0], i2)
        send_q[l, 1] = centred(first, i2)
        send_q[l, 2] = centred(jnp.maximum(col_m[2], col_m[3]), i2)
        up_2 = [(send_q.at[l, pl.ds(0, 2)], halo_q.at[l, pl.ds(1, 2)], 34 + 2 * l), mean_up(i2)]
        down_2 = [(send_q.at[l, 2], halo_q.at[l, 0], 35 + 2 * l), mean_down(i2)]
        send(up_2, down_2)
        if l == 0:
            for p in mid_pair:
                send_t[0, p] = centred(nexts[0, p], i2)
                send_t[1, p] = centred(nexts[3, p], i2)
            up_t = [(send_t.at[0], halo_t.at[1], 38)]
            down_t = [(send_t.at[1], halo_t.at[0], 39)]
            send(up_t, down_t)
        reduce_middle(i2)
        if l == 1:
            scale, shift, _, _ = scale_shift(i1, None)

            def finish_fine(r):
                for q in range(4):
                    spat[pl.ds(q * K, K), :] = affine(fines[r, q], scale, shift).astype(BF16)
                fine_out[0, r] = jnp.dot(
                    back_f[...], spat[pl.ds(0, 4 * K), :], preferred_element_type=F32
                ).astype(BF16)

            each(8, finish_fine)
        receive(up_2, down_2)
        mean_above, mean_below = norm[i2, 3], norm[i2, 4]
        pool_t[0] = jnp.maximum(flat(tiles(halo_q[l, 0].astype(F32)) + mean_above), col_m[0])
        pool_t[2] = jnp.maximum(
            jnp.maximum(col_m[2], col_m[3]), flat(tiles(halo_q[l, 1].astype(F32)) + mean_below)
        )
        pool_t[3] = flat(tiles(halo_q[l, 2].astype(F32)) + mean_below)
        reduce_end(i2, counts[1])

        scale, shift, _, _ = scale_shift(i2, w_up)
        for e in range(4):
            act_t[e, 0] = flat(
                silu_of_double(tiles(base_t[e]) + (tiles(pool_t[e]) * scale + shift))
            )
        masked_edges(act_t, 3)
        stats = convolve(act_t, tops, i3, 2, 1, 2, 2)
        reduce_start(i3, stats, 2 * 48)
        scale, shift, shift_above, shift_below = scale_shift(i2, None)
        if l == 0:
            send_c[0] = centred(tops[0, 0], i3)
            send_c[1] = centred(tops[1, 0], i3)
            up_3 = [(send_c.at[0], halo_c.at[1], 40), mean_up(i3)]
            down_3 = [(send_c.at[1], halo_c.at[0], 41), mean_down(i3)]
            send(up_3, down_3)
            up_f = [(send_f.at[0], halo_f.at[1], 32)]
            down_f = [(send_f.at[1], halo_f.at[0], 33)]
            send(up_f, down_f)
            reduce_middle(i3)
            receive(up_t, down_t)
            for p in mid_pair:
                mid_in[0, p] = affine(halo_t[0, p], scale, shift_above)
                mid_in[5, p] = affine(halo_t[1, p], scale, shift_below)

            def normalize_mid(e):
                for p in mid_pair:
                    mid_in[e + 1, p] = affine(nexts[e, p], scale, shift)

            each(4, normalize_mid)
            receive(up_3, down_3)
            reduce_end(i3, counts[2])
        else:
            reduce_middle(i3)

            def finish_mid(r):
                for p in mid_pair:
                    spat[pl.ds(p * K, K), :] = affine(nexts[r, p], scale, shift).astype(BF16)
                mid_out[0, r] = jnp.dot(
                    back_m[...], spat[pl.ds(0, 2 * K), :], preferred_element_type=F32
                ).astype(BF16)

            each(4, finish_mid)
            reduce_end(i3, counts[2])
            scale, shift, _, _ = scale_shift(i3, None)
            for e in range(2):
                top_out[0, e] = affine(tops[e, 0], scale, shift).astype(BF16)

    @pl.when(has_above)
    def _():
        for src, _, slot in sends_up:
            wait_bytes(src, halo_s.at[slot])

    @pl.when(has_below)
    def _():
        for src, _, slot in sends_down:
            wait_bytes(src, halo_s.at[slot])

    @pl.when(jnp.logical_not(is_hub))
    def _():
        for index in range(8):
            wait_bytes(slots(plane, 0, 16), plane_s.at[index])

    @pl.when(is_hub)
    def _():
        for index in range(8):
            wait_bytes(slots(plane, 0, 15), plane_s.at[index])
            wait_bytes(slots(ring, 0, 15), ring_s.at[index])


def store_kernel(fine, mid, top, fine_out, mid_out, top_out, sems):
    copies = [
        pltpu.make_async_copy(src, dst, sems.at[i])
        for i, (src, dst) in enumerate(((fine, fine_out), (mid, mid_out), (top, top_out)))
    ]
    for copy in copies:
        copy.start()
    for copy in copies:
        copy.wait()


def body(
    fine_level,
    middle_level,
    coarse_level,
    two_input_weights,
    three_input_weights,
    depthwise,
    pointwise,
    bn_gain,
    bn_bias,
):
    devices = lax.axis_size(BATCH) * lax.axis_size("rows")
    counts = tuple(
        float(a.shape[0] * a.shape[1] * a.shape[2] * devices)
        for a in (fine_level, middle_level, coarse_level)
    )
    any_space = pl.BlockSpec(memory_space=pl.ANY)
    smem = pl.BlockSpec(memory_space=pltpu.SMEM)
    vmem = pltpu.VMEM
    dma = pltpu.SemaphoreType.DMA
    scratch = [
        vmem((10, 192, C), BF16),
        vmem((6, 96, C), BF16),
        vmem((4, 48, C), BF16),
        vmem((2, 3, 3, 4, C), BF16),
        vmem((2, 4, C, C), BF16),
        vmem((2, 4, C), F32),
        vmem((2, 4, C), F32),
        vmem((8, 9, 8, C), F32),
        vmem((192, 192), BF16),
        vmem((96, 96), BF16),
        vmem((192, 192), BF16),
        vmem((96, 96), BF16),
        vmem((10, 4, K, C), F32),
        vmem((10, 4, K, C), F32),
        vmem((6, 2, K, C), F32),
        vmem((6, 2, K, C), F32),
        vmem((6, 2, K, C), F32),
        vmem((4, K, C), F32),
        vmem((4, K, C), F32),
        vmem((4, 1, K, C), F32),
        vmem((6, 2, K, C), F32),
        vmem((4, 4, 2, K, C), F32),
        vmem((2, 8, 4, K, C), F32),
        vmem((2, 2, 1, K, C), F32),
        vmem((8, 2, K, C), F32),
        vmem((4, K, C), F32),
        vmem((6, 2, K, C), F32),
        vmem((4, K, C), F32),
        vmem((4 * 192, C), BF16),
        vmem((8, 5, 8, C), F32),
        vmem((2, 2, 2, K, C), BF16),
        vmem((2, 2, 2, K, C), BF16),
        vmem((2, 3, 2, K, C), BF16),
        vmem((2, 3, 2, K, C), BF16),
        vmem((2, 4, K, C), BF16),
        vmem((2, 4, K, C), BF16),
        vmem((2, 3, K, C), BF16),
        vmem((2, 3, K, C), BF16),
        vmem((2, 2, K, C), BF16),
        vmem((2, 2, K, C), BF16),
        vmem((2, K, C), BF16),
        vmem((2, K, C), BF16),
        vmem((8 * 8, 8, 128), F32),
        vmem((8 * 32, 8, 128), F32),
        dma((9,)),
        dma((8,)),
        dma((8,)),
        dma((8,)),
        dma((8,)),
        dma((42,)),
        dma((42,)),
    ]
    levels = (fine_level, middle_level, coarse_level)
    results = pl.pallas_call(
        functools.partial(kernel, counts),
        out_shape=tuple(vmem(a.shape, BF16) for a in levels),
        in_specs=[any_space] * 3 + [smem] * 2 + [any_space] * 4,
        out_specs=(pl.BlockSpec(memory_space=vmem),) * 3,
        scratch_shapes=scratch,
        name="bifpn",
        compiler_params=pltpu.CompilerParams(
            collective_id=0, has_side_effects=True, vmem_limit_bytes=60 * 1024 * 1024
        ),
    )(
        fine_level,
        middle_level,
        coarse_level,
        jnp.transpose(two_input_weights, (0, 2, 1)),
        three_input_weights,
        jnp.transpose(depthwise, (0, 2, 3, 1, 4)),
        pointwise,
        bn_gain,
        bn_bias,
    )
    return pl.pallas_call(
        store_kernel,
        out_shape=tuple(jax.ShapeDtypeStruct(a.shape, BF16) for a in levels),
        in_specs=[pl.BlockSpec(memory_space=vmem)] * 3,
        out_specs=(any_space,) * 3,
        scratch_shapes=[dma((3,))],
        name="store",
    )(*(pltpu.with_memory_space_constraint(one, vmem) for one in results))


def solution(mesh):
    split = Mesh(
        mesh.devices.reshape(4, 4, 2, mesh.shape["rows"]), ("batch_0", "batch_1", "batch_2", "rows")
    )
    level = P(BATCH, "rows", None, None)
    return jax.shard_map(
        body,
        mesh=split,
        in_specs=(level,) * 3 + (P(),) * 6,
        out_specs=(level,) * 3,
        check_vma=False,
    )
```

```python
import functools

import jax
import jax.numpy as jnp
from jax import lax
from jax.experimental import pallas as pl
from jax.experimental.pallas import tpu as pltpu
from jax.sharding import Mesh
from jax.sharding import PartitionSpec as P

LAYERS = 2
BATCH = ("batch_0", "batch_1", "batch_2")
MESH_ID = pl.DeviceIdType.MESH
HUB = 1
C = 384
K = 48
LOW = -1e30
EPS = 1e-05
F32 = jnp.float32
BF16 = jnp.bfloat16


def ring_distance(d, n):
    return min(d, n - d)


Z_OFFSETS = sorted(range(1, 8), key=lambda d: -ring_distance(d, 8))
XY_OFFSETS = sorted(
    [(a, b) for a in range(4) for b in range(4) if (a, b) != (0, 0)],
    key=lambda o: -(ring_distance(o[0], 4) + ring_distance(o[1], 4)),
)


def tiles(x):
    return x.reshape(x.shape[0] // 8, 8, x.shape[1])


def flat(x):
    return x.reshape(x.shape[0] * x.shape[1], x.shape[2])


def shifted_down(x):
    rolled = pltpu.roll(x, 1, axis=0)
    return jnp.where(lax.broadcasted_iota(jnp.int32, x.shape, 0) == 0, 0.0, rolled)


def shifted_up(x, fill):
    rolled = pltpu.roll(x, x.shape[0] - 1, axis=0)
    at_end = lax.broadcasted_iota(jnp.int32, x.shape, 0) == x.shape[0] - 1
    return jnp.where(at_end, fill, rolled)


def silu_of_double(h):
    return h + h * jnp.tanh(h)


def wait_bytes(ref, sem):
    pltpu.make_async_copy(ref, ref, sem).wait()


def kernel(counts, *refs):
    pl.run_scoped(
        functools.partial(layer_pair, counts, refs),
        act_f=pltpu.VMEM((10, 4, K, C), BF16),
        act_m=pltpu.VMEM((6, 2, K, C), BF16),
        act_t=pltpu.VMEM((4, 1, K, C), BF16),
        dwb=pltpu.VMEM((8, 9, 16, C), BF16),
        spat=pltpu.VMEM((4 * 192, C), BF16),
    )


def layer_pair(counts, refs, act_f, act_m, act_t, dwb, spat):
    (
        fine_hbm,
        mid_hbm,
        top_hbm,
        w2,
        w3,
        dw_hbm,
        pw_hbm,
        gain_hbm,
        bias_hbm,
        fine_out,
        mid_out,
        top_out,
        fine_nat,
        mid_nat,
        top_nat,
        dw_in,
        pw,
        gain,
        bias,
        perm_f,
        perm_m,
        back_f,
        back_m,
        base_f,
        mid_in,
        base_m,
        top_in,
        base_t,
        lifted,
        raw_m,
        raw_f,
        raw_t,
        col_f,
        col_m,
        pool_m,
        pool_t,
        norm,
        halo_m,
        halo_a,
        send_a,
        send_m,
        halo_p,
        send_p,
        halo_f,
        send_f,
        halo_q,
        send_q,
        halo_t,
        send_t,
        halo_c,
        send_c,
        ring,
        plane,
        in_sem,
        ring_s,
        ring_r,
        plane_s,
        plane_r,
        halo_s,
        halo_r,
    ) = refs
    y, x = lax.axis_index("batch_0"), lax.axis_index("batch_1")
    core, z = lax.axis_index("batch_2"), lax.axis_index("rows")
    in_plane = core * 16 + y * 4 + x
    is_hub = core == HUB
    has_above, has_below = z > 0, z < 7

    barrier = pltpu.get_barrier_semaphore()

    def greet(**device):
        pl.semaphore_signal(barrier, inc=1, device_id=device, device_id_type=MESH_ID)

    for d in range(8):
        for c in range(2):
            if d:
                greet(batch_2=lax.rem(core + c, 2), rows=lax.rem(z + d, 8))
    for a in range(4):
        for b in range(4):
            for c in range(2):
                if (a, b, c) != (0, 0, 0):
                    greet(
                        batch_0=lax.rem(y + a, 4),
                        batch_1=lax.rem(x + b, 4),
                        batch_2=lax.rem(core + c, 2),
                    )

    loads = {
        "top": pltpu.make_async_copy(top_hbm.at[0], top_nat.at[pl.ds(1, 2)], in_sem.at[0]),
        "mid": pltpu.make_async_copy(mid_hbm.at[0], mid_nat.at[pl.ds(1, 4)], in_sem.at[1]),
        "dw": pltpu.make_async_copy(dw_hbm, dw_in, in_sem.at[2]),
        "fine": pltpu.make_async_copy(fine_hbm.at[0], fine_nat.at[pl.ds(1, 8)], in_sem.at[3]),
        "pw": pltpu.make_async_copy(pw_hbm.at[0, 0], pw.at[0, 0], in_sem.at[4]),
        "pw_0": pltpu.make_async_copy(pw_hbm.at[0, pl.ds(1, 3)], pw.at[0, pl.ds(1, 3)], in_sem.at[7]),
        "pw_1": pltpu.make_async_copy(pw_hbm.at[1], pw.at[1], in_sem.at[8]),
        "gain": pltpu.make_async_copy(gain_hbm, gain, in_sem.at[5]),
        "bias": pltpu.make_async_copy(bias_hbm, bias, in_sem.at[6]),
    }
    for load in loads.values():
        load.start()

    def permutation(ref, back, parts):
        n = parts * K
        row = lax.broadcasted_iota(jnp.int32, (n, n), 0)
        col = lax.broadcasted_iota(jnp.int32, (n, n), 1)
        ref[...] = jnp.where(lax.rem(row, K) * parts + lax.div(row, K) == col, 1.0, 0.0).astype(BF16)
        back[...] = jnp.where(lax.rem(col, K) * parts + lax.div(col, K) == row, 1.0, 0.0).astype(
            BF16
        )

    permutation(perm_m, back_m, 2)
    permutation(perm_f, back_f, 4)

    def zeroed(ref):
        ref[...] = jnp.zeros(ref.shape, ref.dtype)

    @pl.when(z == 0)
    def _():
        for ref in (fine_nat.at[0], mid_nat.at[0], top_nat.at[0]):
            zeroed(ref)
        for l in range(LAYERS):
            for ref in (halo_m.at[l, 0], halo_p.at[l, 0], halo_q.at[l, 0]):
                zeroed(ref)
        for ref in (halo_f.at[0], halo_t.at[0], halo_c.at[0], halo_a.at[0]):
            zeroed(ref)
        for node in range(8):
            zeroed(norm.at[node, 3])

    @pl.when(z == 7)
    def _():
        for ref in (fine_nat.at[9], mid_nat.at[5], top_nat.at[3]):
            zeroed(ref)
        for l in range(LAYERS):
            zeroed(halo_m.at[l, 1])
            for s in (1, 2):
                for ref in (halo_p.at[l, s], halo_q.at[l, s]):
                    ref[...] = jnp.full(ref.shape, LOW, BF16)
        for ref in (halo_f.at[1], halo_t.at[1], halo_c.at[1], halo_a.at[1]):
            zeroed(ref)
        for node in range(8):
            zeroed(norm.at[node, 4])

    loads["dw"].wait()
    for l in range(LAYERS):
        for i in range(3):
            for j in range(3):
                taps = dw_in[l, i, j].astype(F32)
                for n in range(4):
                    dwb[l * 4 + n, 3 * i + j] = jnp.broadcast_to(taps[n : n + 1], (16, C)).astype(BF16)

    above = {"rows": jnp.maximum(z - 1, 0)}
    below = {"rows": jnp.minimum(z + 1, 7)}

    def to_above(src, dst, slot):
        return pltpu.make_async_remote_copy(
            src, dst, halo_s.at[slot], halo_r.at[slot], device_id=above, device_id_type=MESH_ID
        )

    def to_below(src, dst, slot):
        return pltpu.make_async_remote_copy(
            src, dst, halo_s.at[slot], halo_r.at[slot], device_id=below, device_id_type=MESH_ID
        )

    sends_up, sends_down = [], []

    def send(up, down):
        @pl.when(has_above)
        def _():
            for one in up:
                to_above(*one).start()

        @pl.when(has_below)
        def _():
            for one in down:
                to_below(*one).start()

        sends_up.extend(up)
        sends_down.extend(down)

    def receive(from_below, from_above):
        @pl.when(has_below)
        def _():
            for _, dst, slot in from_below:
                wait_bytes(dst, halo_r.at[slot])

        @pl.when(has_above)
        def _():
            for _, dst, slot in from_above:
                wait_bytes(dst, halo_r.at[slot])

    def halves(weights):
        spread = [jnp.full((8, C), 1.0, F32) * w for w in weights]
        acc = spread[0]
        for one in spread[1:]:
            acc = acc + one
        acc = acc + 0.0001
        return [0.5 * one / acc for one in spread]

    def two(l, n):
        return halves([w2[l, 0, n], w2[l, 1, n]])

    def three(l):
        return halves([w3[l, 0], w3[l, 1], w3[l, 2]])

    def convolve(
        act, raw, index, height, planes, step_rows, dot_rows, order=None, before_rest=None
    ):
        lanes = planes * K

        def row_of(base, dr):
            return base + dr if order is None else order[dr]

        def depthwise(r, at):
            for c in range(3):
                cs = pl.ds(c * 128, 128)
                taps = [dwb[index, t, :, cs] for t in range(9)]
                sums = []
                for q in range(planes):
                    rows = [act[r + i, q, :, cs].reshape(K // 16, 16, 128) for i in range(3)]
                    sums.append(
                        [
                            flat(rows[0] * taps[j] + rows[1] * taps[3 + j] + rows[2] * taps[6 + j])
                            for j in range(3)
                        ]
                    )
                left_edge = shifted_down(sums[planes - 1][0].astype(F32)).astype(BF16)
                right_edge = shifted_up(sums[0][2].astype(F32), 0.0).astype(BF16)
                for q in range(planes):
                    left = sums[q - 1][0] if q else left_edge
                    right = sums[q + 1][2] if q + 1 < planes else right_edge
                    spat[pl.ds(at + q * K, K), cs] = left + sums[q][1] + right

        def step(s, carry):
            total, squares = carry
            for first in range(0, step_rows, dot_rows):
                if first and before_rest is not None:
                    before_rest()
                for dr in range(first, first + dot_rows):
                    depthwise(row_of(s * step_rows, dr), dr * lanes)
                out = jnp.dot(
                    spat[pl.ds(first * lanes, dot_rows * lanes), :],
                    pw[index // 4, index % 4],
                    preferred_element_type=F32,
                )
                for dr in range(dot_rows):
                    for q in range(planes):
                        at = dr * lanes + q * K
                        raw[row_of(s * step_rows, first + dr), q] = out[at : at + K]
                out = tiles(out)
                total, squares = total + jnp.sum(out, axis=0), squares + jnp.sum(out * out, axis=0)
            return total, squares

        start = (jnp.zeros((8, C), F32), jnp.zeros((8, C), F32))
        return lax.fori_loop(0, height // step_rows, step, start)

    def slots(buffer, first, n):
        return buffer.at[pl.ds(first, n), pl.ds(0, 6)]

    def push(buffer, slot, sent, received, **device):
        pltpu.make_async_remote_copy(
            buffer.at[slot, pl.ds(0, 6)],
            buffer.at[slot, pl.ds(0, 6)],
            sent,
            received,
            device_id=device,
            device_id_type=MESH_ID,
        ).start()

    def added(buffer, first, n):
        terms = [buffer[first + k, 0:6] for k in range(n)]
        while len(terms) > 1:
            terms = [terms[k] + terms[k + 1] for k in range(0, len(terms), 2)]
        return terms[0]

    def plane_device(a, b):
        return {"batch_0": lax.rem(y + a, 4), "batch_1": lax.rem(x + b, 4)}

    def reduce_start(index, stats, local_count):
        total, squares = stats
        total = jnp.sum(total, axis=0, keepdims=True)
        squares = jnp.sum(squares, axis=0, keepdims=True)
        mine = index * 32 + in_plane
        for c in range(3):
            plane[mine, c : c + 1, :] = total[:, c * 128 : (c + 1) * 128]
            plane[mine, 3 + c : 4 + c, :] = squares[:, c * 128 : (c + 1) * 128]
        norm[index, 2] = jnp.broadcast_to(total * (1.0 / local_count), (8, C))

        for a, b in XY_OFFSETS:
            push(
                plane, mine, plane_s.at[index], plane_r.at[index], **plane_device(a, b), batch_2=HUB
            )

        @pl.when(jnp.logical_not(is_hub))
        def _():
            push(plane, mine, plane_s.at[index], plane_r.at[index], batch_2=HUB)

    def reduce_middle(index):
        @pl.when(is_hub)
        def _():
            wait_bytes(slots(plane, index * 32, 31), plane_r.at[index])
            mine = index * 8 + z
            ring[mine, 0:6] = added(plane, index * 32, 32)
            for d in Z_OFFSETS:
                at = lax.rem(z + d, 8)
                push(ring, mine, ring_s.at[index], ring_r.at[index], batch_2=1 - HUB, rows=at)
                push(ring, mine, ring_s.at[index], ring_r.at[index], rows=at)
            push(ring, mine, ring_s.at[index], ring_r.at[index], batch_2=1 - HUB)

    def reduce_end(index, count):
        @pl.when(is_hub)
        def _():
            wait_bytes(slots(ring, index * 8, 7), ring_r.at[index])

        @pl.when(jnp.logical_not(is_hub))
        def _():
            wait_bytes(slots(ring, index * 8, 8), ring_r.at[index])

        acc = added(ring, index * 8, 8) * (1.0 / count)
        l, n = index // 4, index % 4
        for c in range(3):
            cs = pl.ds(c * 128, 128)
            center = acc[c : c + 1]
            spread = acc[3 + c : 4 + c] - center * center
            scale = gain[l, n : n + 1, cs] * lax.rsqrt(spread + EPS)
            shift = bias[l, n : n + 1, cs] - center * scale
            norm[index, 0, :, cs] = jnp.broadcast_to(scale, (8, 128))
            norm[index, 1, :, cs] = jnp.broadcast_to(shift, (8, 128))

    def centred(value, index):
        return flat(tiles(value) - norm[index, 2]).astype(BF16)

    def mean_up(index):
        return (norm.at[index, 2], norm.at[index, 4], 8 + 2 * index)

    def mean_down(index):
        return (norm.at[index, 2], norm.at[index, 3], 9 + 2 * index)

    def scale_shift(index, weight):
        scale, shift = norm[index, 0], norm[index, 1]
        if weight is not None:
            scale, shift = scale * weight, shift * weight
        shift_above = norm[index, 3] * scale + shift
        shift_below = norm[index, 4] * scale + shift
        return scale, shift, shift_above, shift_below

    def affine(value, scale, shift):
        return flat(tiles(value.astype(F32)) * scale + shift)

    def masked_edges(act, last):
        @pl.when(z == 0)
        def _():
            zeroed(act.at[0])

        @pl.when(z == 7)
        def _():
            zeroed(act.at[last])

    def each(n, fn):
        def step(i, _):
            fn(i)
            return 0

        lax.fori_loop(0, n, step, 0)

    def column_pool(load, planes):
        out = []
        for p in range(max(planes // 2, 1)):
            x0, x1 = load(2 * p), load(2 * p + 1)
            x2 = load(2 * p + 2) if 2 * p + 2 < planes else shifted_up(load(0), LOW)
            out.append(jnp.maximum(jnp.maximum(x0, x1), x2))
        return out

    mid_pair = range(2)

    for l in range(LAYERS):
        i0, i1, i2, i3 = (4 * l + n for n in range(4))
        mids = raw_m.at[2 * l]
        fines = raw_f.at[l]
        nexts = raw_m.at[2 * l + 1]
        tops = raw_t.at[l]

        own, up = two(l, 0)

        def join_0(e, act):
            t = tiles(top_in[lax.div(e + 1, 2)]) * up
            for p in mid_pair:
                act[e, p] = flat(silu_of_double(tiles(mid_in[e, p]) * own + t)).astype(BF16)

        if l == 0:

            def place_mid(e):
                out = jnp.dot(perm_m[...], mid_nat[e], preferred_element_type=F32)
                for p in mid_pair:
                    mid_in[e, p] = out[p * K : (p + 1) * K]

            loads["top"].wait()
            loads["mid"].wait()
            for e in (1, 2):
                top_in[e] = top_nat[e].astype(F32)

            def own_row(e):
                place_mid(e + 1)
                join_0(e + 1, act_m)

            each(4, own_row)
            send_a[0] = act_m[1]
            send_a[1] = act_m[4]
            pl.semaphore_wait(barrier, 14 + 31)
            up_a = [(send_a.at[0], halo_a.at[1], 6)]
            down_a = [(send_a.at[1], halo_a.at[0], 7)]
            send(up_a, down_a)
            loads["fine"].wait()
            fine_up = [(fine_nat.at[1], fine_nat.at[9], 4)]
            fine_down = [(fine_nat.at[8], fine_nat.at[0], 5)]
            send(fine_up, fine_down)
            loads["pw"].wait()

            def edge_rows():
                receive(up_a, down_a)
                act_m[0] = halo_a[0]
                act_m[5] = halo_a[1]

            stats = convolve(act_m, mids, i0, 4, 2, 4, 2, (1, 2, 0, 3), edge_rows)
        else:
            scale, shift, shift_above, shift_below = scale_shift(3, None)
            for e in range(4):
                if e == 0:
                    top_in[e] = affine(halo_c[0], scale, shift_above)
                elif e == 3:
                    top_in[e] = affine(halo_c[1], scale, shift_below)
                else:
                    top_in[e] = affine(raw_t[0, e - 1, 0], scale, shift)
            each(6, lambda e: join_0(e, act_m))
            masked_edges(act_m, 5)
            stats = convolve(act_m, mids, i0, 4, 2, 4, 2)
        reduce_start(i0, stats, 4 * 96)
        for p in mid_pair:
            send_m[l, 0, p] = centred(mids[0, p], i0)
            send_m[l, 1, p] = centred(mids[3, p], i0)
        up_0 = [(send_m.at[l, 0], halo_m.at[l, 1], 24 + 2 * l), mean_up(i0)]
        down_0 = [(send_m.at[l, 1], halo_m.at[l, 0], 25 + 2 * l), mean_down(i0)]
        send(up_0, down_0)
        if l == 0:
            first_up = [
                (mid_nat.at[1], mid_nat.at[5], 0),
                (top_nat.at[1], top_nat.at[3], 1),
            ]
            first_down = [
                (mid_nat.at[4], mid_nat.at[0], 2),
                (top_nat.at[2], top_nat.at[0], 3),
            ]
            send(first_up, first_down)
        reduce_middle(i0)

        own, up = two(l, 1)
        if l == 0:
            receive(fine_up, fine_down)

            def place_fine(e):
                out = jnp.dot(perm_f[...], fine_nat[e], preferred_element_type=F32)
                for q in range(4):
                    base_f[e, q] = flat(tiles(out[q * K : (q + 1) * K]) * own)

            each(10, place_fine)
            receive(first_up, first_down)
            place_mid(0)
            place_mid(5)
            for e in (0, 3):
                top_in[e] = top_nat[e].astype(F32)
        else:
            receive(up_f, down_f)
            scale, shift, shift_above, shift_below = scale_shift(1, own)

            def place_fine(e):
                for q in range(4):
                    base_f[e + 1, q] = affine(raw_f[0, e, q], scale, shift)

            each(8, place_fine)
            for q in range(4):
                base_f[0, q] = affine(halo_f[0, q], scale, shift_above)
                base_f[9, q] = affine(halo_f[1, q], scale, shift_below)

        receive(up_0, down_0)
        if l == 0:
            for name in ("pw_0", "pw_1", "gain", "bias"):
                loads[name].wait()
        reduce_end(i0, counts[1])

        scale, shift, shift_above, shift_below = scale_shift(i0, up)
        for p in mid_pair:
            lifted[0, p] = affine(halo_m[l, 0, p], scale, shift_above)
            lifted[5, p] = affine(halo_m[l, 1, p], scale, shift_below)

        def lift(e):
            for p in mid_pair:
                lifted[e + 1, p] = affine(mids[e, p], scale, shift)

        each(4, lift)

        def join_1(e):
            m = lax.div(e + 1, 2)
            for p in mid_pair:
                t = lifted[m, p]
                for q in (2 * p, 2 * p + 1):
                    act_f[e, q] = silu_of_double(base_f[e, q] + t).astype(BF16)

        each(10, join_1)
        masked_edges(act_f, 9)
        stats = convolve(act_f, fines, i1, 8, 4, 4, 1)
        reduce_start(i1, stats, 8 * 192)

        def pool_columns(r):
            for p, out in enumerate(column_pool(lambda q: fines[r, q], 4)):
                col_f[r, p] = out

        each(8, pool_columns)
        for p in mid_pair:
            first = jnp.maximum(jnp.maximum(col_f[0, p], col_f[1, p]), col_f[2, p])
            pool_m[1, p] = first
            send_p[l, 0, p] = centred(col_f[0, p], i1)
            send_p[l, 1, p] = centred(first, i1)
            send_p[l, 2, p] = centred(jnp.maximum(col_f[6, p], col_f[7, p]), i1)
        up_1 = [(send_p.at[l, pl.ds(0, 2)], halo_p.at[l, pl.ds(1, 2)], 28 + 2 * l), mean_up(i1)]
        down_1 = [(send_p.at[l, 2], halo_p.at[l, 0], 29 + 2 * l), mean_down(i1)]
        send(up_1, down_1)
        reduce_middle(i1)
        if l == 0:
            for q in range(4):
                send_f[0, q] = centred(fines[0, q], i1)
                send_f[1, q] = centred(fines[7, q], i1)

        w_mid, w_down, w_pool = three(l)
        scale, shift, shift_above, shift_below = scale_shift(i0, w_down)

        def known(e, value, one_shift):
            for p in mid_pair:
                base_m[e, p] = flat(
                    tiles(mid_in[e, p]) * w_mid + tiles(value(p).astype(F32)) * scale + one_shift
                )

        known(0, lambda p: halo_m[l, 0, p], shift_above)
        known(5, lambda p: halo_m[l, 1, p], shift_below)
        each(4, lambda e: known(e + 1, lambda p: mids[e, p], shift))
        w_top, w_up = two(l, 2)
        for e in range(4):
            base_t[e] = flat(tiles(top_in[e]) * w_top)
        for i in (1, 2):
            for p in mid_pair:
                pool_m[i + 1, p] = jnp.maximum(
                    jnp.maximum(col_f[2 * i, p], col_f[2 * i + 1, p]), col_f[2 * i + 2, p]
                )
        receive(up_1, down_1)
        mean_above, mean_below = norm[i1, 3], norm[i1, 4]
        for p in mid_pair:
            pool_m[0, p] = jnp.maximum(
                flat(tiles(halo_p[l, 0, p].astype(F32)) + mean_above), col_f[0, p]
            )
            pool_m[4, p] = jnp.maximum(
                jnp.maximum(col_f[6, p], col_f[7, p]),
                flat(tiles(halo_p[l, 1, p].astype(F32)) + mean_below),
            )
            pool_m[5, p] = flat(tiles(halo_p[l, 2, p].astype(F32)) + mean_below)
        reduce_end(i1, counts[0])

        scale, shift, _, _ = scale_shift(i1, w_pool)

        def join_2(e):
            for p in mid_pair:
                act_m[e, p] = flat(
                    silu_of_double(tiles(base_m[e, p]) + (tiles(pool_m[e, p]) * scale + shift))
                ).astype(BF16)

        each(6, join_2)
        masked_edges(act_m, 5)
        stats = convolve(act_m, nexts, i2, 4, 2, 4, 2)
        reduce_start(i2, stats, 4 * 96)
        for r in range(4):
            col_m[r] = column_pool(lambda q: nexts[r, q], 2)[0]
        first = jnp.maximum(jnp.maximum(col_m[0], col_m[1]), col_m[2])
        pool_t[1] = first
        send_q[l, 0] = centred(col_m[0], i2)
        send_q[l, 1] = centred(first, i2)
        send_q[l, 2] = centred(jnp.maximum(col_m[2], col_m[3]), i2)
        up_2 = [(send_q.at[l, pl.ds(0, 2)], halo_q.at[l, pl.ds(1, 2)], 34 + 2 * l), mean_up(i2)]
        down_2 = [(send_q.at[l, 2], halo_q.at[l, 0], 35 + 2 * l), mean_down(i2)]
        send(up_2, down_2)
        if l == 0:
            for p in mid_pair:
                send_t[0, p] = centred(nexts[0, p], i2)
                send_t[1, p] = centred(nexts[3, p], i2)
            up_t = [(send_t.at[0], halo_t.at[1], 38)]
            down_t = [(send_t.at[1], halo_t.at[0], 39)]
            send(up_t, down_t)
        reduce_middle(i2)
        if l == 1:
            scale, shift, _, _ = scale_shift(i1, None)

            def finish_fine(r):
                for q in range(4):
                    spat[pl.ds(q * K, K), :] = affine(fines[r, q], scale, shift).astype(BF16)
                fine_out[0, r] = jnp.dot(
                    back_f[...], spat[pl.ds(0, 4 * K), :], preferred_element_type=F32
                ).astype(BF16)

            each(8, finish_fine)
        receive(up_2, down_2)
        mean_above, mean_below = norm[i2, 3], norm[i2, 4]
        pool_t[0] = jnp.maximum(flat(tiles(halo_q[l, 0].astype(F32)) + mean_above), col_m[0])
        pool_t[2] = jnp.maximum(
            jnp.maximum(col_m[2], col_m[3]), flat(tiles(halo_q[l, 1].astype(F32)) + mean_below)
        )
        pool_t[3] = flat(tiles(halo_q[l, 2].astype(F32)) + mean_below)
        reduce_end(i2, counts[1])

        scale, shift, _, _ = scale_shift(i2, w_up)
        for e in range(4):
            act_t[e, 0] = flat(
                silu_of_double(tiles(base_t[e]) + (tiles(pool_t[e]) * scale + shift))
            ).astype(BF16)
        masked_edges(act_t, 3)
        stats = convolve(act_t, tops, i3, 2, 1, 2, 2)
        reduce_start(i3, stats, 2 * 48)
        scale, shift, shift_above, shift_below = scale_shift(i2, None)
        if l == 0:
            send_c[0] = centred(tops[0, 0], i3)
            send_c[1] = centred(tops[1, 0], i3)
            up_3 = [(send_c.at[0], halo_c.at[1], 40), mean_up(i3)]
            down_3 = [(send_c.at[1], halo_c.at[0], 41), mean_down(i3)]
            send(up_3, down_3)
            up_f = [(send_f.at[0], halo_f.at[1], 32)]
            down_f = [(send_f.at[1], halo_f.at[0], 33)]
            send(up_f, down_f)
            reduce_middle(i3)
            receive(up_t, down_t)
            for p in mid_pair:
                mid_in[0, p] = affine(halo_t[0, p], scale, shift_above)
                mid_in[5, p] = affine(halo_t[1, p], scale, shift_below)

            def normalize_mid(e):
                for p in mid_pair:
                    mid_in[e + 1, p] = affine(nexts[e, p], scale, shift)

            each(4, normalize_mid)
            receive(up_3, down_3)
            reduce_end(i3, counts[2])
        else:
            reduce_middle(i3)

            def finish_mid(r):
                for p in mid_pair:
                    spat[pl.ds(p * K, K), :] = affine(nexts[r, p], scale, shift).astype(BF16)
                mid_out[0, r] = jnp.dot(
                    back_m[...], spat[pl.ds(0, 2 * K), :], preferred_element_type=F32
                ).astype(BF16)

            each(4, finish_mid)
            reduce_end(i3, counts[2])
            scale, shift, _, _ = scale_shift(i3, None)
            for e in range(2):
                top_out[0, e] = affine(tops[e, 0], scale, shift).astype(BF16)

    @pl.when(has_above)
    def _():
        for src, _, slot in sends_up:
            wait_bytes(src, halo_s.at[slot])

    @pl.when(has_below)
    def _():
        for src, _, slot in sends_down:
            wait_bytes(src, halo_s.at[slot])

    @pl.when(jnp.logical_not(is_hub))
    def _():
        for index in range(8):
            wait_bytes(slots(plane, 0, 16), plane_s.at[index])

    @pl.when(is_hub)
    def _():
        for index in range(8):
            wait_bytes(slots(plane, 0, 15), plane_s.at[index])
            wait_bytes(slots(ring, 0, 15), ring_s.at[index])


def store_kernel(fine, mid, top, fine_out, mid_out, top_out, sems):
    copies = [
        pltpu.make_async_copy(src, dst, sems.at[i])
        for i, (src, dst) in enumerate(((fine, fine_out), (mid, mid_out), (top, top_out)))
    ]
    for copy in copies:
        copy.start()
    for copy in copies:
        copy.wait()


def body(
    fine_level,
    middle_level,
    coarse_level,
    two_input_weights,
    three_input_weights,
    depthwise,
    pointwise,
    bn_gain,
    bn_bias,
):
    devices = lax.axis_size(BATCH) * lax.axis_size("rows")
    counts = tuple(
        float(a.shape[0] * a.shape[1] * a.shape[2] * devices)
        for a in (fine_level, middle_level, coarse_level)
    )
    any_space = pl.BlockSpec(memory_space=pl.ANY)
    smem = pl.BlockSpec(memory_space=pltpu.SMEM)
    vmem = pltpu.VMEM
    dma = pltpu.SemaphoreType.DMA
    scratch = [
        vmem((10, 192, C), BF16),
        vmem((6, 96, C), BF16),
        vmem((4, 48, C), BF16),
        vmem((2, 3, 3, 4, C), BF16),
        vmem((2, 4, C, C), BF16),
        vmem((2, 4, C), F32),
        vmem((2, 4, C), F32),
        vmem((192, 192), BF16),
        vmem((96, 96), BF16),
        vmem((192, 192), BF16),
        vmem((96, 96), BF16),
        vmem((10, 4, K, C), F32),
        vmem((6, 2, K, C), F32),
        vmem((6, 2, K, C), F32),
        vmem((4, K, C), F32),
        vmem((4, K, C), F32),
        vmem((6, 2, K, C), F32),
        vmem((4, 4, 2, K, C), F32),
        vmem((2, 8, 4, K, C), F32),
        vmem((2, 2, 1, K, C), F32),
        vmem((8, 2, K, C), F32),
        vmem((4, K, C), F32),
        vmem((6, 2, K, C), F32),
        vmem((4, K, C), F32),
        vmem((8, 5, 8, C), F32),
        vmem((2, 2, 2, K, C), BF16),
        vmem((2, 2, K, C), BF16),
        vmem((2, 2, K, C), BF16),
        vmem((2, 2, 2, K, C), BF16),
        vmem((2, 3, 2, K, C), BF16),
        vmem((2, 3, 2, K, C), BF16),
        vmem((2, 4, K, C), BF16),
        vmem((2, 4, K, C), BF16),
        vmem((2, 3, K, C), BF16),
        vmem((2, 3, K, C), BF16),
        vmem((2, 2, K, C), BF16),
        vmem((2, 2, K, C), BF16),
        vmem((2, K, C), BF16),
        vmem((2, K, C), BF16),
        vmem((8 * 8, 8, 128), F32),
        vmem((8 * 32, 8, 128), F32),
        dma((9,)),
        dma((8,)),
        dma((8,)),
        dma((8,)),
        dma((8,)),
        dma((42,)),
        dma((42,)),
    ]
    levels = (fine_level, middle_level, coarse_level)
    results = pl.pallas_call(
        functools.partial(kernel, counts),
        out_shape=tuple(vmem(a.shape, BF16) for a in levels),
        in_specs=[any_space] * 3 + [smem] * 2 + [any_space] * 4,
        out_specs=(pl.BlockSpec(memory_space=vmem),) * 3,
        scratch_shapes=scratch,
        name="bifpn",
        compiler_params=pltpu.CompilerParams(
            collective_id=0, has_side_effects=True, vmem_limit_bytes=60 * 1024 * 1024
        ),
    )(
        fine_level,
        middle_level,
        coarse_level,
        jnp.transpose(two_input_weights, (0, 2, 1)),
        three_input_weights,
        jnp.transpose(depthwise, (0, 2, 3, 1, 4)),
        pointwise,
        bn_gain,
        bn_bias,
    )
    return pl.pallas_call(
        store_kernel,
        out_shape=tuple(jax.ShapeDtypeStruct(a.shape, BF16) for a in levels),
        in_specs=[pl.BlockSpec(memory_space=vmem)] * 3,
        out_specs=(any_space,) * 3,
        scratch_shapes=[dma((3,))],
        name="store",
    )(*(pltpu.with_memory_space_constraint(one, vmem) for one in results))


def solution(mesh):
    split = Mesh(
        mesh.devices.reshape(4, 4, 2, mesh.shape["rows"]), ("batch_0", "batch_1", "batch_2", "rows")
    )
    level = P(BATCH, "rows", None, None)
    return jax.shard_map(
        body,
        mesh=split,
        in_specs=(level,) * 3 + (P(),) * 6,
        out_specs=(level,) * 3,
        check_vma=False,
    )
```

```python
import functools

import jax
import jax.numpy as jnp
from jax import lax
from jax.experimental import pallas as pl
from jax.experimental.pallas import tpu as pltpu
from jax.sharding import Mesh
from jax.sharding import PartitionSpec as P

LAYERS = 2
BATCH = ("batch_0", "batch_1", "batch_2")
MESH_ID = pl.DeviceIdType.MESH
HUB = 1
C = 384
K = 48
LOW = -1e30
EPS = 1e-05
F32 = jnp.float32
BF16 = jnp.bfloat16


def ring_distance(d, n):
    return min(d, n - d)


Z_OFFSETS = sorted(range(1, 8), key=lambda d: -ring_distance(d, 8))
XY_OFFSETS = sorted(
    [(a, b) for a in range(4) for b in range(4) if (a, b) != (0, 0)],
    key=lambda o: -(ring_distance(o[0], 4) + ring_distance(o[1], 4)),
)


def tiles(x):
    return x.reshape(x.shape[0] // 8, 8, x.shape[1])


def flat(x):
    return x.reshape(x.shape[0] * x.shape[1], x.shape[2])


def shifted_down(x):
    rolled = pltpu.roll(x, 1, axis=0)
    return jnp.where(lax.broadcasted_iota(jnp.int32, x.shape, 0) == 0, 0.0, rolled)


def shifted_up(x, fill):
    rolled = pltpu.roll(x, x.shape[0] - 1, axis=0)
    at_end = lax.broadcasted_iota(jnp.int32, x.shape, 0) == x.shape[0] - 1
    return jnp.where(at_end, fill, rolled)


def silu_of_double(h):
    return h + h * jnp.tanh(h)


def wait_bytes(ref, sem):
    pltpu.make_async_copy(ref, ref, sem).wait()


def kernel(counts, *refs):
    pl.run_scoped(
        functools.partial(layer_pair, counts, refs),
        act_f=pltpu.VMEM((10, 4, K, C), BF16),
        act_m=pltpu.VMEM((6, 2, K, C), BF16),
        act_t=pltpu.VMEM((4, 1, K, C), BF16),
        dwb=pltpu.VMEM((8, 9, 16, C), BF16),
        spat=pltpu.VMEM((4 * 192, C), BF16),
    )


def layer_pair(counts, refs, act_f, act_m, act_t, dwb, spat):
    (
        fine_hbm,
        mid_hbm,
        top_hbm,
        w2,
        w3,
        dw_hbm,
        pw_hbm,
        gain_hbm,
        bias_hbm,
        fine_out,
        mid_out,
        top_out,
        fine_nat,
        mid_nat,
        top_nat,
        dw_in,
        pw,
        gain,
        bias,
        perm_f,
        perm_m,
        back_f,
        back_m,
        base_f,
        mid_in,
        base_m,
        top_in,
        base_t,
        lifted,
        raw_m,
        raw_f,
        raw_t,
        col_f,
        col_m,
        pool_m,
        pool_t,
        norm,
        halo_m,
        halo_a,
        send_a,
        send_m,
        halo_p,
        send_p,
        halo_f,
        send_f,
        halo_q,
        send_q,
        halo_t,
        send_t,
        halo_c,
        send_c,
        ring,
        plane,
        in_sem,
        ring_s,
        ring_r,
        plane_s,
        plane_r,
        halo_s,
        halo_r,
        rounds,
    ) = refs
    y, x = lax.axis_index("batch_0"), lax.axis_index("batch_1")
    core, z = lax.axis_index("batch_2"), lax.axis_index("rows")
    in_plane = core * 16 + y * 4 + x
    is_hub = core == HUB
    has_above, has_below = z > 0, z < 7

    barrier = pltpu.get_barrier_semaphore()
    one_step = [
        {axis: lax.rem(lax.axis_index(axis) + d, n)}
        for axis, n in (("rows", 8), ("batch_0", 4), ("batch_1", 4))
        for d in (1, n - 1)
    ]

    def greet(semaphore, devices):
        for device in devices:
            pl.semaphore_signal(semaphore, inc=1, device_id=device, device_id_type=MESH_ID)

    greet(barrier, one_step + [{"batch_2": 1 - core}])

    def entry_round(k):
        if k:
            pl.semaphore_wait(rounds.at[k - 1], 6)
        else:
            pl.semaphore_wait(barrier, 7)
        if k < 3:
            greet(rounds.at[k], one_step)

    def entry_end():
        @pl.when(is_hub)
        def _():
            greet(rounds.at[3], [{"batch_2": 1 - core}])

        @pl.when(jnp.logical_not(is_hub))
        def _():
            pl.semaphore_wait(rounds.at[3], 1)

    loads = {
        "top": pltpu.make_async_copy(top_hbm.at[0], top_nat.at[pl.ds(1, 2)], in_sem.at[0]),
        "mid": pltpu.make_async_copy(mid_hbm.at[0], mid_nat.at[pl.ds(1, 4)], in_sem.at[1]),
        "dw": pltpu.make_async_copy(dw_hbm, dw_in, in_sem.at[2]),
        "fine": pltpu.make_async_copy(fine_hbm.at[0], fine_nat.at[pl.ds(1, 8)], in_sem.at[3]),
        "pw": pltpu.make_async_copy(pw_hbm.at[0, 0], pw.at[0, 0], in_sem.at[4]),
        "pw_0": pltpu.make_async_copy(pw_hbm.at[0, pl.ds(1, 3)], pw.at[0, pl.ds(1, 3)], in_sem.at[7]),
        "pw_1": pltpu.make_async_copy(pw_hbm.at[1], pw.at[1], in_sem.at[8]),
        "gain": pltpu.make_async_copy(gain_hbm, gain, in_sem.at[5]),
        "bias": pltpu.make_async_copy(bias_hbm, bias, in_sem.at[6]),
    }
    for load in loads.values():
        load.start()

    def zeroed(ref):
        ref[...] = jnp.zeros(ref.shape, ref.dtype)

    def permutation(ref, parts, inverse):
        n = parts * K
        row = lax.broadcasted_iota(jnp.int32, (n, n), 0)
        col = lax.broadcasted_iota(jnp.int32, (n, n), 1)
        if inverse:
            row, col = col, row
        ref[...] = jnp.where(lax.rem(row, K) * parts + lax.div(row, K) == col, 1.0, 0.0).astype(BF16)

    above = {"rows": jnp.maximum(z - 1, 0)}
    below = {"rows": jnp.minimum(z + 1, 7)}

    def to_above(src, dst, slot):
        return pltpu.make_async_remote_copy(
            src, dst, halo_s.at[slot], halo_r.at[slot], device_id=above, device_id_type=MESH_ID
        )

    def to_below(src, dst, slot):
        return pltpu.make_async_remote_copy(
            src, dst, halo_s.at[slot], halo_r.at[slot], device_id=below, device_id_type=MESH_ID
        )

    sends_up, sends_down = [], []

    def send(up, down):
        @pl.when(has_above)
        def _():
            for one in up:
                to_above(*one).start()

        @pl.when(has_below)
        def _():
            for one in down:
                to_below(*one).start()

        sends_up.extend(up)
        sends_down.extend(down)

    def receive(from_below, from_above):
        @pl.when(has_below)
        def _():
            for _, dst, slot in from_below:
                wait_bytes(dst, halo_r.at[slot])

        @pl.when(has_above)
        def _():
            for _, dst, slot in from_above:
                wait_bytes(dst, halo_r.at[slot])

    def halves(weights):
        spread = [jnp.full((8, C), 1.0, F32) * w for w in weights]
        acc = spread[0]
        for one in spread[1:]:
            acc = acc + one
        acc = acc + 0.0001
        return [0.5 * one / acc for one in spread]

    def two(l, n):
        return halves([w2[l, 0, n], w2[l, 1, n]])

    def three(l):
        return halves([w3[l, 0], w3[l, 1], w3[l, 2]])

    def spread_taps():
        loads["dw"].wait()
        for l in range(LAYERS):
            for i in range(3):
                for j in range(3):
                    taps = dw_in[l, i, j].astype(F32)
                    for n in range(4):
                        dwb[l * 4 + n, 3 * i + j] = jnp.broadcast_to(taps[n : n + 1], (16, C)).astype(BF16)

    def fill_edges():
        @pl.when(z == 0)
        def _():
            for ref in (fine_nat.at[0], mid_nat.at[0], top_nat.at[0]):
                zeroed(ref)
            for l in range(LAYERS):
                for ref in (halo_m.at[l, 0], halo_p.at[l, 0], halo_q.at[l, 0]):
                    zeroed(ref)
            for ref in (halo_f.at[0], halo_t.at[0], halo_c.at[0], halo_a.at[0]):
                zeroed(ref)
            for node in range(8):
                zeroed(norm.at[node, 3])

        @pl.when(z == 7)
        def _():
            for ref in (fine_nat.at[9], mid_nat.at[5], top_nat.at[3]):
                zeroed(ref)
            for l in range(LAYERS):
                zeroed(halo_m.at[l, 1])
                for s in (1, 2):
                    for ref in (halo_p.at[l, s], halo_q.at[l, s]):
                        ref[...] = jnp.full(ref.shape, LOW, BF16)
            for ref in (halo_f.at[1], halo_t.at[1], halo_c.at[1], halo_a.at[1]):
                zeroed(ref)
            for node in range(8):
                zeroed(norm.at[node, 4])

    def convolve(
        act, raw, index, height, planes, step_rows, dot_rows, order=None, before_rest=None
    ):
        lanes = planes * K

        def row_of(base, dr):
            return base + dr if order is None else order[dr]

        def depthwise(r, at):
            for c in range(3):
                cs = pl.ds(c * 128, 128)
                taps = [dwb[index, t, :, cs] for t in range(9)]
                sums = []
                for q in range(planes):
                    rows = [act[r + i, q, :, cs].reshape(K // 16, 16, 128) for i in range(3)]
                    sums.append(
                        [
                            flat(rows[0] * taps[j] + rows[1] * taps[3 + j] + rows[2] * taps[6 + j])
                            for j in range(3)
                        ]
                    )
                left_edge = shifted_down(sums[planes - 1][0].astype(F32)).astype(BF16)
                right_edge = shifted_up(sums[0][2].astype(F32), 0.0).astype(BF16)
                for q in range(planes):
                    left = sums[q - 1][0] if q else left_edge
                    right = sums[q + 1][2] if q + 1 < planes else right_edge
                    spat[pl.ds(at + q * K, K), cs] = left + sums[q][1] + right

        def step(s, carry):
            total, squares = carry
            for first in range(0, step_rows, dot_rows):
                if first and before_rest is not None:
                    before_rest()
                for dr in range(first, first + dot_rows):
                    depthwise(row_of(s * step_rows, dr), dr * lanes)
                out = jnp.dot(
                    spat[pl.ds(first * lanes, dot_rows * lanes), :],
                    pw[index // 4, index % 4],
                    preferred_element_type=F32,
                )
                for dr in range(dot_rows):
                    for q in range(planes):
                        at = dr * lanes + q * K
                        raw[row_of(s * step_rows, first + dr), q] = out[at : at + K]
                out = tiles(out)
                total, squares = total + jnp.sum(out, axis=0), squares + jnp.sum(out * out, axis=0)
            return total, squares

        start = (jnp.zeros((8, C), F32), jnp.zeros((8, C), F32))
        return lax.fori_loop(0, height // step_rows, step, start)

    def slots(buffer, first, n):
        return buffer.at[pl.ds(first, n), pl.ds(0, 6)]

    def push(buffer, slot, sent, received, **device):
        pltpu.make_async_remote_copy(
            buffer.at[slot, pl.ds(0, 6)],
            buffer.at[slot, pl.ds(0, 6)],
            sent,
            received,
            device_id=device,
            device_id_type=MESH_ID,
        ).start()

    def added(buffer, first, n):
        terms = [buffer[first + k, 0:6] for k in range(n)]
        while len(terms) > 1:
            terms = [terms[k] + terms[k + 1] for k in range(0, len(terms), 2)]
        return terms[0]

    def plane_device(a, b):
        return {"batch_0": lax.rem(y + a, 4), "batch_1": lax.rem(x + b, 4)}

    def reduce_start(index, stats, local_count):
        total, squares = stats
        total = jnp.sum(total, axis=0, keepdims=True)
        squares = jnp.sum(squares, axis=0, keepdims=True)
        mine = index * 32 + in_plane
        for c in range(3):
            plane[mine, c : c + 1, :] = total[:, c * 128 : (c + 1) * 128]
            plane[mine, 3 + c : 4 + c, :] = squares[:, c * 128 : (c + 1) * 128]
        norm[index, 2] = jnp.broadcast_to(total * (1.0 / local_count), (8, C))

        for a, b in XY_OFFSETS:
            push(
                plane, mine, plane_s.at[index], plane_r.at[index], **plane_device(a, b), batch_2=HUB
            )

        @pl.when(jnp.logical_not(is_hub))
        def _():
            push(plane, mine, plane_s.at[index], plane_r.at[index], batch_2=HUB)

    def reduce_middle(index):
        @pl.when(is_hub)
        def _():
            wait_bytes(slots(plane, index * 32, 31), plane_r.at[index])
            mine = index * 8 + z
            ring[mine, 0:6] = added(plane, index * 32, 32)
            for d in Z_OFFSETS:
                at = lax.rem(z + d, 8)
                push(ring, mine, ring_s.at[index], ring_r.at[index], batch_2=1 - HUB, rows=at)
                push(ring, mine, ring_s.at[index], ring_r.at[index], rows=at)
            push(ring, mine, ring_s.at[index], ring_r.at[index], batch_2=1 - HUB)

    def reduce_end(index, count):
        @pl.when(is_hub)
        def _():
            wait_bytes(slots(ring, index * 8, 7), ring_r.at[index])

        @pl.when(jnp.logical_not(is_hub))
        def _():
            wait_bytes(slots(ring, index * 8, 8), ring_r.at[index])

        acc = added(ring, index * 8, 8) * (1.0 / count)
        l, n = index // 4, index % 4
        for c in range(3):
            cs = pl.ds(c * 128, 128)
            center = acc[c : c + 1]
            spread = acc[3 + c : 4 + c] - center * center
            scale = gain[l, n : n + 1, cs] * lax.rsqrt(spread + EPS)
            shift = bias[l, n : n + 1, cs] - center * scale
            norm[index, 0, :, cs] = jnp.broadcast_to(scale, (8, 128))
            norm[index, 1, :, cs] = jnp.broadcast_to(shift, (8, 128))

    def centred(value, index):
        return flat(tiles(value) - norm[index, 2]).astype(BF16)

    def mean_up(index):
        return (norm.at[index, 2], norm.at[index, 4], 8 + 2 * index)

    def mean_down(index):
        return (norm.at[index, 2], norm.at[index, 3], 9 + 2 * index)

    def scale_shift(index, weight):
        scale, shift = norm[index, 0], norm[index, 1]
        if weight is not None:
            scale, shift = scale * weight, shift * weight
        shift_above = norm[index, 3] * scale + shift
        shift_below = norm[index, 4] * scale + shift
        return scale, shift, shift_above, shift_below

    def affine(value, scale, shift):
        return flat(tiles(value.astype(F32)) * scale + shift)

    def masked_edges(act, last):
        @pl.when(z == 0)
        def _():
            zeroed(act.at[0])

        @pl.when(z == 7)
        def _():
            zeroed(act.at[last])

    def each(n, fn, at_once=1):
        def step(i, _):
            for k in range(at_once):
                fn(i * at_once + k)
            return 0

        lax.fori_loop(0, n // at_once, step, 0)

    def column_pool(load, planes):
        out = []
        for p in range(max(planes // 2, 1)):
            x0, x1 = load(2 * p), load(2 * p + 1)
            x2 = load(2 * p + 2) if 2 * p + 2 < planes else shifted_up(load(0), LOW)
            out.append(jnp.maximum(jnp.maximum(x0, x1), x2))
        return out

    mid_pair = range(2)

    for l in range(LAYERS):
        i0, i1, i2, i3 = (4 * l + n for n in range(4))
        mids = raw_m.at[2 * l]
        fines = raw_f.at[l]
        nexts = raw_m.at[2 * l + 1]
        tops = raw_t.at[l]

        own, up = two(l, 0)

        def join_0(e, act):
            t = tiles(top_in[lax.div(e + 1, 2)]) * up
            for p in mid_pair:
                act[e, p] = flat(silu_of_double(tiles(mid_in[e, p]) * own + t)).astype(BF16)

        if l == 0:

            def place_mid(e):
                out = jnp.dot(perm_m[...], mid_nat[e], preferred_element_type=F32)
                for p in mid_pair:
                    mid_in[e, p] = out[p * K : (p + 1) * K]

            permutation(perm_m, 2, False)
            loads["top"].wait()
            loads["mid"].wait()
            for e in (1, 2):
                top_in[e] = top_nat[e].astype(F32)
            for e in (1, 4):
                place_mid(e)
                join_0(e, act_m)
            send_a[0] = act_m[1]
            send_a[1] = act_m[4]
            entry_round(0)
            up_a = [(send_a.at[0], halo_a.at[1], 6)]
            down_a = [(send_a.at[1], halo_a.at[0], 7)]
            send(up_a, down_a)
            for e in (2, 3):
                place_mid(e)
                join_0(e, act_m)
            fill_edges()
            spread_taps()
            loads["fine"].wait()
            fine_up = [(fine_nat.at[1], fine_nat.at[9], 4)]
            fine_down = [(fine_nat.at[8], fine_nat.at[0], 5)]
            send(fine_up, fine_down)
            loads["pw"].wait()

            def edge_rows():
                permutation(perm_f, 4, False)
                for k in (1, 2, 3):
                    entry_round(k)
                entry_end()
                receive(up_a, down_a)
                act_m[0] = halo_a[0]
                act_m[5] = halo_a[1]

            stats = convolve(act_m, mids, i0, 4, 2, 4, 2, (1, 2, 0, 3), edge_rows)
        else:
            scale, shift, shift_above, shift_below = scale_shift(3, None)
            for e in range(4):
                if e == 0:
                    top_in[e] = affine(halo_c[0], scale, shift_above)
                elif e == 3:
                    top_in[e] = affine(halo_c[1], scale, shift_below)
                else:
                    top_in[e] = affine(raw_t[0, e - 1, 0], scale, shift)
            each(6, lambda e: join_0(e, act_m), 3)
            masked_edges(act_m, 5)
            stats = convolve(act_m, mids, i0, 4, 2, 4, 2)
        reduce_start(i0, stats, 4 * 96)
        for p in mid_pair:
            send_m[l, 0, p] = centred(mids[0, p], i0)
            send_m[l, 1, p] = centred(mids[3, p], i0)
        up_0 = [(send_m.at[l, 0], halo_m.at[l, 1], 24 + 2 * l), mean_up(i0)]
        down_0 = [(send_m.at[l, 1], halo_m.at[l, 0], 25 + 2 * l), mean_down(i0)]
        send(up_0, down_0)
        if l == 0:
            first_up = [
                (mid_nat.at[1], mid_nat.at[5], 0),
                (top_nat.at[1], top_nat.at[3], 1),
            ]
            first_down = [
                (mid_nat.at[4], mid_nat.at[0], 2),
                (top_nat.at[2], top_nat.at[0], 3),
            ]
            send(first_up, first_down)
        reduce_middle(i0)

        own, up = two(l, 1)
        if l == 0:
            receive(fine_up, fine_down)

            def place_fine(e):
                out = jnp.dot(perm_f[...], fine_nat[e], preferred_element_type=F32)
                for q in range(4):
                    base_f[e, q] = flat(tiles(out[q * K : (q + 1) * K]) * own)

            each(10, place_fine)
            receive(first_up, first_down)
            place_mid(0)
            place_mid(5)
            for e in (0, 3):
                top_in[e] = top_nat[e].astype(F32)
        else:
            receive(up_f, down_f)
            scale, shift, shift_above, shift_below = scale_shift(1, own)

            def place_fine(e):
                for q in range(4):
                    base_f[e + 1, q] = affine(raw_f[0, e, q], scale, shift)

            each(8, place_fine)
            for q in range(4):
                base_f[0, q] = affine(halo_f[0, q], scale, shift_above)
                base_f[9, q] = affine(halo_f[1, q], scale, shift_below)

        receive(up_0, down_0)
        if l == 0:
            for name in ("pw_0", "pw_1", "gain", "bias"):
                loads[name].wait()
        reduce_end(i0, counts[1])

        scale, shift, shift_above, shift_below = scale_shift(i0, up)
        for p in mid_pair:
            lifted[0, p] = affine(halo_m[l, 0, p], scale, shift_above)
            lifted[5, p] = affine(halo_m[l, 1, p], scale, shift_below)

        def lift(e):
            for p in mid_pair:
                lifted[e + 1, p] = affine(mids[e, p], scale, shift)

        each(4, lift, 2)

        def join_1(e):
            m = lax.div(e + 1, 2)
            for p in mid_pair:
                t = lifted[m, p]
                for q in (2 * p, 2 * p + 1):
                    act_f[e, q] = silu_of_double(base_f[e, q] + t).astype(BF16)

        each(10, join_1, 2)
        masked_edges(act_f, 9)
        stats = convolve(act_f, fines, i1, 8, 4, 4, 2)
        reduce_start(i1, stats, 8 * 192)

        def pool_columns(r):
            for p, out in enumerate(column_pool(lambda q: fines[r, q], 4)):
                col_f[r, p] = out

        each(8, pool_columns)
        for p in mid_pair:
            first = jnp.maximum(jnp.maximum(col_f[0, p], col_f[1, p]), col_f[2, p])
            pool_m[1, p] = first
            send_p[l, 0, p] = centred(col_f[0, p], i1)
            send_p[l, 1, p] = centred(first, i1)
            send_p[l, 2, p] = centred(jnp.maximum(col_f[6, p], col_f[7, p]), i1)
        up_1 = [(send_p.at[l, pl.ds(0, 2)], halo_p.at[l, pl.ds(1, 2)], 28 + 2 * l), mean_up(i1)]
        down_1 = [(send_p.at[l, 2], halo_p.at[l, 0], 29 + 2 * l), mean_down(i1)]
        send(up_1, down_1)
        reduce_middle(i1)
        if l == 0:
            for q in range(4):
                send_f[0, q] = centred(fines[0, q], i1)
                send_f[1, q] = centred(fines[7, q], i1)

        w_mid, w_down, w_pool = three(l)
        scale, shift, shift_above, shift_below = scale_shift(i0, w_down)

        def known(e, value, one_shift):
            for p in mid_pair:
                base_m[e, p] = flat(
                    tiles(mid_in[e, p]) * w_mid + tiles(value(p).astype(F32)) * scale + one_shift
                )

        known(0, lambda p: halo_m[l, 0, p], shift_above)
        known(5, lambda p: halo_m[l, 1, p], shift_below)
        each(4, lambda e: known(e + 1, lambda p: mids[e, p], shift))
        w_top, w_up = two(l, 2)
        for e in range(4):
            base_t[e] = flat(tiles(top_in[e]) * w_top)
        for i in (1, 2):
            for p in mid_pair:
                pool_m[i + 1, p] = jnp.maximum(
                    jnp.maximum(col_f[2 * i, p], col_f[2 * i + 1, p]), col_f[2 * i + 2, p]
                )
        receive(up_1, down_1)
        mean_above, mean_below = norm[i1, 3], norm[i1, 4]
        for p in mid_pair:
            pool_m[0, p] = jnp.maximum(
                flat(tiles(halo_p[l, 0, p].astype(F32)) + mean_above), col_f[0, p]
            )
            pool_m[4, p] = jnp.maximum(
                jnp.maximum(col_f[6, p], col_f[7, p]),
                flat(tiles(halo_p[l, 1, p].astype(F32)) + mean_below),
            )
            pool_m[5, p] = flat(tiles(halo_p[l, 2, p].astype(F32)) + mean_below)
        reduce_end(i1, counts[0])

        scale, shift, _, _ = scale_shift(i1, w_pool)

        def join_2(e):
            for p in mid_pair:
                act_m[e, p] = flat(
                    silu_of_double(tiles(base_m[e, p]) + (tiles(pool_m[e, p]) * scale + shift))
                ).astype(BF16)

        each(6, join_2, 3)
        masked_edges(act_m, 5)
        stats = convolve(act_m, nexts, i2, 4, 2, 4, 2)
        reduce_start(i2, stats, 4 * 96)
        for r in range(4):
            col_m[r] = column_pool(lambda q: nexts[r, q], 2)[0]
        first = jnp.maximum(jnp.maximum(col_m[0], col_m[1]), col_m[2])
        pool_t[1] = first
        send_q[l, 0] = centred(col_m[0], i2)
        send_q[l, 1] = centred(first, i2)
        send_q[l, 2] = centred(jnp.maximum(col_m[2], col_m[3]), i2)
        up_2 = [(send_q.at[l, pl.ds(0, 2)], halo_q.at[l, pl.ds(1, 2)], 34 + 2 * l), mean_up(i2)]
        down_2 = [(send_q.at[l, 2], halo_q.at[l, 0], 35 + 2 * l), mean_down(i2)]
        send(up_2, down_2)
        if l == 0:
            for p in mid_pair:
                send_t[0, p] = centred(nexts[0, p], i2)
                send_t[1, p] = centred(nexts[3, p], i2)
            up_t = [(send_t.at[0], halo_t.at[1], 38)]
            down_t = [(send_t.at[1], halo_t.at[0], 39)]
            send(up_t, down_t)
        reduce_middle(i2)
        if l == 1:
            scale, shift, _, _ = scale_shift(i1, None)

            permutation(back_f, 4, True)
            permutation(back_m, 2, True)

            def finish_fine(r):
                for q in range(4):
                    spat[pl.ds(q * K, K), :] = affine(fines[r, q], scale, shift).astype(BF16)
                fine_out[0, r] = jnp.dot(
                    back_f[...], spat[pl.ds(0, 4 * K), :], preferred_element_type=F32
                ).astype(BF16)

            each(8, finish_fine)
        receive(up_2, down_2)
        mean_above, mean_below = norm[i2, 3], norm[i2, 4]
        pool_t[0] = jnp.maximum(flat(tiles(halo_q[l, 0].astype(F32)) + mean_above), col_m[0])
        pool_t[2] = jnp.maximum(
            jnp.maximum(col_m[2], col_m[3]), flat(tiles(halo_q[l, 1].astype(F32)) + mean_below)
        )
        pool_t[3] = flat(tiles(halo_q[l, 2].astype(F32)) + mean_below)
        reduce_end(i2, counts[1])

        scale, shift, _, _ = scale_shift(i2, w_up)
        for e in range(4):
            act_t[e, 0] = flat(
                silu_of_double(tiles(base_t[e]) + (tiles(pool_t[e]) * scale + shift))
            ).astype(BF16)
        masked_edges(act_t, 3)
        stats = convolve(act_t, tops, i3, 2, 1, 2, 2)
        reduce_start(i3, stats, 2 * 48)
        scale, shift, shift_above, shift_below = scale_shift(i2, None)
        if l == 0:
            send_c[0] = centred(tops[0, 0], i3)
            send_c[1] = centred(tops[1, 0], i3)
            up_3 = [(send_c.at[0], halo_c.at[1], 40), mean_up(i3)]
            down_3 = [(send_c.at[1], halo_c.at[0], 41), mean_down(i3)]
            send(up_3, down_3)
            up_f = [(send_f.at[0], halo_f.at[1], 32)]
            down_f = [(send_f.at[1], halo_f.at[0], 33)]
            send(up_f, down_f)
            reduce_middle(i3)
            receive(up_t, down_t)
            for p in mid_pair:
                mid_in[0, p] = affine(halo_t[0, p], scale, shift_above)
                mid_in[5, p] = affine(halo_t[1, p], scale, shift_below)

            def normalize_mid(e):
                for p in mid_pair:
                    mid_in[e + 1, p] = affine(nexts[e, p], scale, shift)

            each(4, normalize_mid)
            receive(up_3, down_3)
            reduce_end(i3, counts[2])
        else:
            reduce_middle(i3)

            def finish_mid(r):
                for p in mid_pair:
                    spat[pl.ds(p * K, K), :] = affine(nexts[r, p], scale, shift).astype(BF16)
                mid_out[0, r] = jnp.dot(
                    back_m[...], spat[pl.ds(0, 2 * K), :], preferred_element_type=F32
                ).astype(BF16)

            each(4, finish_mid)
            reduce_end(i3, counts[2])
            scale, shift, _, _ = scale_shift(i3, None)
            for e in range(2):
                top_out[0, e] = affine(tops[e, 0], scale, shift).astype(BF16)

    @pl.when(has_above)
    def _():
        for src, _, slot in sends_up:
            wait_bytes(src, halo_s.at[slot])

    @pl.when(has_below)
    def _():
        for src, _, slot in sends_down:
            wait_bytes(src, halo_s.at[slot])

    @pl.when(jnp.logical_not(is_hub))
    def _():
        for index in range(8):
            wait_bytes(slots(plane, 0, 16), plane_s.at[index])

    @pl.when(is_hub)
    def _():
        for index in range(8):
            wait_bytes(slots(plane, 0, 15), plane_s.at[index])
            wait_bytes(slots(ring, 0, 15), ring_s.at[index])


def store_kernel(fine, mid, top, fine_out, mid_out, top_out, sems):
    copies = [
        pltpu.make_async_copy(src, dst, sems.at[i])
        for i, (src, dst) in enumerate(((fine, fine_out), (mid, mid_out), (top, top_out)))
    ]
    for copy in copies:
        copy.start()
    for copy in copies:
        copy.wait()


def body(
    fine_level,
    middle_level,
    coarse_level,
    two_input_weights,
    three_input_weights,
    depthwise,
    pointwise,
    bn_gain,
    bn_bias,
):
    devices = lax.axis_size(BATCH) * lax.axis_size("rows")
    counts = tuple(
        float(a.shape[0] * a.shape[1] * a.shape[2] * devices)
        for a in (fine_level, middle_level, coarse_level)
    )
    any_space = pl.BlockSpec(memory_space=pl.ANY)
    smem = pl.BlockSpec(memory_space=pltpu.SMEM)
    vmem = pltpu.VMEM
    dma = pltpu.SemaphoreType.DMA
    scratch = [
        vmem((10, 192, C), BF16),
        vmem((6, 96, C), BF16),
        vmem((4, 48, C), BF16),
        vmem((2, 3, 3, 4, C), BF16),
        vmem((2, 4, C, C), BF16),
        vmem((2, 4, C), F32),
        vmem((2, 4, C), F32),
        vmem((192, 192), BF16),
        vmem((96, 96), BF16),
        vmem((192, 192), BF16),
        vmem((96, 96), BF16),
        vmem((10, 4, K, C), F32),
        vmem((6, 2, K, C), F32),
        vmem((6, 2, K, C), F32),
        vmem((4, K, C), F32),
        vmem((4, K, C), F32),
        vmem((6, 2, K, C), F32),
        vmem((4, 4, 2, K, C), F32),
        vmem((2, 8, 4, K, C), F32),
        vmem((2, 2, 1, K, C), F32),
        vmem((8, 2, K, C), F32),
        vmem((4, K, C), F32),
        vmem((6, 2, K, C), F32),
        vmem((4, K, C), F32),
        vmem((8, 5, 8, C), F32),
        vmem((2, 2, 2, K, C), BF16),
        vmem((2, 2, K, C), BF16),
        vmem((2, 2, K, C), BF16),
        vmem((2, 2, 2, K, C), BF16),
        vmem((2, 3, 2, K, C), BF16),
        vmem((2, 3, 2, K, C), BF16),
        vmem((2, 4, K, C), BF16),
        vmem((2, 4, K, C), BF16),
        vmem((2, 3, K, C), BF16),
        vmem((2, 3, K, C), BF16),
        vmem((2, 2, K, C), BF16),
        vmem((2, 2, K, C), BF16),
        vmem((2, K, C), BF16),
        vmem((2, K, C), BF16),
        vmem((8 * 8, 8, 128), F32),
        vmem((8 * 32, 8, 128), F32),
        dma((9,)),
        dma((8,)),
        dma((8,)),
        dma((8,)),
        dma((8,)),
        dma((42,)),
        dma((42,)),
        pltpu.SemaphoreType.REGULAR((4,)),
    ]
    levels = (fine_level, middle_level, coarse_level)
    results = pl.pallas_call(
        functools.partial(kernel, counts),
        out_shape=tuple(vmem(a.shape, BF16) for a in levels),
        in_specs=[any_space] * 3 + [smem] * 2 + [any_space] * 4,
        out_specs=(pl.BlockSpec(memory_space=vmem),) * 3,
        scratch_shapes=scratch,
        name="bifpn",
        compiler_params=pltpu.CompilerParams(
            collective_id=0, has_side_effects=True, vmem_limit_bytes=60 * 1024 * 1024
        ),
    )(
        fine_level,
        middle_level,
        coarse_level,
        jnp.transpose(two_input_weights, (0, 2, 1)),
        three_input_weights,
        jnp.transpose(depthwise, (0, 2, 3, 1, 4)),
        pointwise,
        bn_gain,
        bn_bias,
    )
    return pl.pallas_call(
        store_kernel,
        out_shape=tuple(jax.ShapeDtypeStruct(a.shape, BF16) for a in levels),
        in_specs=[pl.BlockSpec(memory_space=vmem)] * 3,
        out_specs=(any_space,) * 3,
        scratch_shapes=[dma((3,))],
        name="store",
    )(*(pltpu.with_memory_space_constraint(one, vmem) for one in results))


def solution(mesh):
    split = Mesh(
        mesh.devices.reshape(4, 4, 2, mesh.shape["rows"]), ("batch_0", "batch_1", "batch_2", "rows")
    )
    level = P(BATCH, "rows", None, None)
    return jax.shard_map(
        body,
        mesh=split,
        in_specs=(level,) * 3 + (P(),) * 6,
        out_specs=(level,) * 3,
        check_vma=False,
    )
```

```python
import functools

import jax
import jax.numpy as jnp
from jax import lax
from jax.experimental import pallas as pl
from jax.experimental.pallas import tpu as pltpu
from jax.sharding import Mesh
from jax.sharding import PartitionSpec as P

LAYERS = 2
BATCH = ("batch_0", "batch_1", "batch_2")
MESH_ID = pl.DeviceIdType.MESH
HUB = 1
C = 384
K = 48
LOW = -1e30
EPS = 1e-05
F32 = jnp.float32
BF16 = jnp.bfloat16


def ring_distance(d, n):
    return min(d, n - d)


Z_OFFSETS = sorted(range(1, 8), key=lambda d: -ring_distance(d, 8))
XY_OFFSETS = sorted(
    [(a, b) for a in range(4) for b in range(4) if (a, b) != (0, 0)],
    key=lambda o: -(ring_distance(o[0], 4) + ring_distance(o[1], 4)),
)


def tiles(x):
    return x.reshape(x.shape[0] // 8, 8, x.shape[1])


def flat(x):
    return x.reshape(x.shape[0] * x.shape[1], x.shape[2])


def shifted_down(x):
    rolled = pltpu.roll(x, 1, axis=0)
    return jnp.where(lax.broadcasted_iota(jnp.int32, x.shape, 0) == 0, 0.0, rolled)


def shifted_up(x, fill):
    rolled = pltpu.roll(x, x.shape[0] - 1, axis=0)
    at_end = lax.broadcasted_iota(jnp.int32, x.shape, 0) == x.shape[0] - 1
    return jnp.where(at_end, fill, rolled)


def silu_of_double(h):
    return h + h * jnp.tanh(h)


def wait_bytes(ref, sem):
    pltpu.make_async_copy(ref, ref, sem).wait()


def kernel(counts, *refs):
    pl.run_scoped(
        functools.partial(layer_pair, counts, refs),
        act_f=pltpu.VMEM((10, 4, K, C), BF16),
        act_m=pltpu.VMEM((6, 2, K, C), BF16),
        act_t=pltpu.VMEM((4, 1, K, C), BF16),
        dwb=pltpu.VMEM((8, 9, 16, C), BF16),
        spat=pltpu.VMEM((8 * 192, C), BF16),
    )


def layer_pair(counts, refs, act_f, act_m, act_t, dwb, spat):
    (
        fine_hbm,
        mid_hbm,
        top_hbm,
        w2,
        w3,
        dw_hbm,
        pw_hbm,
        gain_hbm,
        bias_hbm,
        fine_out,
        mid_out,
        top_out,
        fine_nat,
        mid_nat,
        top_nat,
        dw_in,
        pw,
        gain,
        bias,
        perm_f,
        perm_m,
        back_f,
        back_m,
        base_f,
        mid_in,
        base_m,
        top_in,
        base_t,
        lifted,
        raw_m,
        raw_f,
        raw_t,
        col_f,
        col_m,
        pool_m,
        pool_t,
        norm,
        halo_m,
        halo_a,
        send_a,
        send_m,
        halo_p,
        send_p,
        halo_f,
        send_f,
        halo_q,
        send_q,
        halo_t,
        send_t,
        halo_c,
        send_c,
        ring,
        plane,
        in_sem,
        ring_s,
        ring_r,
        plane_s,
        plane_r,
        halo_s,
        halo_r,
        rounds,
    ) = refs
    y, x = lax.axis_index("batch_0"), lax.axis_index("batch_1")
    core, z = lax.axis_index("batch_2"), lax.axis_index("rows")
    in_plane = core * 16 + y * 4 + x
    is_hub = core == HUB
    has_above, has_below = z > 0, z < 7

    barrier = pltpu.get_barrier_semaphore()
    one_step = [
        {axis: lax.rem(lax.axis_index(axis) + d, n)}
        for axis, n in (("rows", 8), ("batch_0", 4), ("batch_1", 4))
        for d in (1, n - 1)
    ]

    def greet(semaphore, devices):
        for device in devices:
            pl.semaphore_signal(semaphore, inc=1, device_id=device, device_id_type=MESH_ID)

    greet(barrier, one_step + [{"batch_2": 1 - core}])

    def entry_round(k):
        if k:
            pl.semaphore_wait(rounds.at[k - 1], 6)
        else:
            pl.semaphore_wait(barrier, 7)
        if k < 3:
            greet(rounds.at[k], one_step)

    def entry_end():
        @pl.when(is_hub)
        def _():
            greet(rounds.at[3], [{"batch_2": 1 - core}])

        @pl.when(jnp.logical_not(is_hub))
        def _():
            pl.semaphore_wait(rounds.at[3], 1)

    loads = {
        "top": pltpu.make_async_copy(top_hbm.at[0], top_nat.at[pl.ds(1, 2)], in_sem.at[0]),
        "mid": pltpu.make_async_copy(mid_hbm.at[0], mid_nat.at[pl.ds(1, 4)], in_sem.at[1]),
        "dw": pltpu.make_async_copy(dw_hbm, dw_in, in_sem.at[2]),
        "fine": pltpu.make_async_copy(fine_hbm.at[0], fine_nat.at[pl.ds(1, 8)], in_sem.at[3]),
        "pw": pltpu.make_async_copy(pw_hbm.at[0, 0], pw.at[0, 0], in_sem.at[4]),
        "pw_0": pltpu.make_async_copy(pw_hbm.at[0, pl.ds(1, 3)], pw.at[0, pl.ds(1, 3)], in_sem.at[7]),
        "pw_1": pltpu.make_async_copy(pw_hbm.at[1], pw.at[1], in_sem.at[8]),
        "gain": pltpu.make_async_copy(gain_hbm, gain, in_sem.at[5]),
        "bias": pltpu.make_async_copy(bias_hbm, bias, in_sem.at[6]),
    }
    for load in loads.values():
        load.start()

    def zeroed(ref):
        ref[...] = jnp.zeros(ref.shape, ref.dtype)

    def permutation(ref, parts, inverse):
        n = parts * K
        row = lax.broadcasted_iota(jnp.int32, (n, n), 0)
        col = lax.broadcasted_iota(jnp.int32, (n, n), 1)
        if inverse:
            row, col = col, row
        ref[...] = jnp.where(lax.rem(row, K) * parts + lax.div(row, K) == col, 1.0, 0.0).astype(BF16)

    above = {"rows": jnp.maximum(z - 1, 0)}
    below = {"rows": jnp.minimum(z + 1, 7)}

    def to_above(src, dst, slot):
        return pltpu.make_async_remote_copy(
            src, dst, halo_s.at[slot], halo_r.at[slot], device_id=above, device_id_type=MESH_ID
        )

    def to_below(src, dst, slot):
        return pltpu.make_async_remote_copy(
            src, dst, halo_s.at[slot], halo_r.at[slot], device_id=below, device_id_type=MESH_ID
        )

    sends_up, sends_down = [], []

    def start_sends(up, down):
        @pl.when(has_above)
        def _():
            for one in up:
                to_above(*one).start()

        @pl.when(has_below)
        def _():
            for one in down:
                to_below(*one).start()

    def send(up, down):
        start_sends(up, down)
        sends_up.extend(up)
        sends_down.extend(down)

    def receive(from_below, from_above):
        @pl.when(has_below)
        def _():
            for _, dst, slot in from_below:
                wait_bytes(dst, halo_r.at[slot])

        @pl.when(has_above)
        def _():
            for _, dst, slot in from_above:
                wait_bytes(dst, halo_r.at[slot])

    def halves(weights):
        spread = [jnp.full((8, C), 1.0, F32) * w for w in weights]
        acc = spread[0]
        for one in spread[1:]:
            acc = acc + one
        acc = acc + 0.0001
        return [0.5 * one / acc for one in spread]

    def two(l, n):
        return halves([w2[l, 0, n], w2[l, 1, n]])

    def three(l):
        return halves([w3[l, 0], w3[l, 1], w3[l, 2]])

    def spread_taps():
        loads["dw"].wait()
        for l in range(LAYERS):
            for i in range(3):
                for j in range(3):
                    taps = dw_in[l, i, j].astype(F32)
                    for n in range(4):
                        dwb[l * 4 + n, 3 * i + j] = jnp.broadcast_to(taps[n : n + 1], (16, C)).astype(BF16)

    def fill_edges():
        @pl.when(z == 0)
        def _():
            for ref in (fine_nat.at[0], mid_nat.at[0], top_nat.at[0]):
                zeroed(ref)
            for l in range(LAYERS):
                for ref in (halo_m.at[l, 0], halo_p.at[l, 0], halo_q.at[l, 0]):
                    zeroed(ref)
            for ref in (halo_f.at[0], halo_t.at[0], halo_c.at[0], halo_a.at[0]):
                zeroed(ref)
            for node in range(8):
                zeroed(norm.at[node, 3])

        @pl.when(z == 7)
        def _():
            for ref in (fine_nat.at[9], mid_nat.at[5], top_nat.at[3]):
                zeroed(ref)
            for l in range(LAYERS):
                zeroed(halo_m.at[l, 1])
                for s in (1, 2):
                    for ref in (halo_p.at[l, s], halo_q.at[l, s]):
                        ref[...] = jnp.full(ref.shape, LOW, BF16)
            for ref in (halo_f.at[1], halo_t.at[1], halo_c.at[1], halo_a.at[1]):
                zeroed(ref)
            for node in range(8):
                zeroed(norm.at[node, 4])

    def convolve(
        act, raw, index, height, planes, step_rows, dot_rows, order=None, before_rest=None
    ):
        lanes = planes * K

        def row_of(base, dr):
            return base + dr if order is None else order[dr]

        def depthwise(r, at):
            for c in range(3):
                cs = pl.ds(c * 128, 128)
                taps = [dwb[index, t, :, cs] for t in range(9)]
                sums = []
                for q in range(planes):
                    rows = [act[r + i, q, :, cs].reshape(K // 16, 16, 128) for i in range(3)]
                    sums.append(
                        [
                            flat(rows[0] * taps[j] + rows[1] * taps[3 + j] + rows[2] * taps[6 + j])
                            for j in range(3)
                        ]
                    )
                left_edge = shifted_down(sums[planes - 1][0].astype(F32)).astype(BF16)
                right_edge = shifted_up(sums[0][2].astype(F32), 0.0).astype(BF16)
                for q in range(planes):
                    left = sums[q - 1][0] if q else left_edge
                    right = sums[q + 1][2] if q + 1 < planes else right_edge
                    spat[pl.ds(at + q * K, K), cs] = left + sums[q][1] + right

        def step(s, carry):
            total, squares = carry
            for first in range(0, step_rows, dot_rows):
                if first and before_rest is not None:
                    before_rest()
                for dr in range(first, first + dot_rows):
                    depthwise(row_of(s * step_rows, dr), dr * lanes)
                out = jnp.dot(
                    spat[pl.ds(first * lanes, dot_rows * lanes), :],
                    pw[index // 4, index % 4],
                    preferred_element_type=F32,
                )
                for dr in range(dot_rows):
                    for q in range(planes):
                        at = dr * lanes + q * K
                        raw[row_of(s * step_rows, first + dr), q] = out[at : at + K]
                out = tiles(out)
                total, squares = total + jnp.sum(out, axis=0), squares + jnp.sum(out * out, axis=0)
            return total, squares

        start = (jnp.zeros((8, C), F32), jnp.zeros((8, C), F32))
        return lax.fori_loop(0, height // step_rows, step, start)

    def slots(buffer, first, n):
        return buffer.at[pl.ds(first, n), pl.ds(0, 6)]

    def push(buffer, slot, sent, received, **device):
        pltpu.make_async_remote_copy(
            buffer.at[slot, pl.ds(0, 6)],
            buffer.at[slot, pl.ds(0, 6)],
            sent,
            received,
            device_id=device,
            device_id_type=MESH_ID,
        ).start()

    def added(buffer, first, n):
        terms = [buffer[first + k, 0:6] for k in range(n)]
        while len(terms) > 1:
            terms = [terms[k] + terms[k + 1] for k in range(0, len(terms), 2)]
        return terms[0]

    def plane_device(a, b):
        return {"batch_0": lax.rem(y + a, 4), "batch_1": lax.rem(x + b, 4)}

    def reduce_start(index, stats, local_count):
        total, squares = stats
        total = jnp.sum(total, axis=0, keepdims=True)
        squares = jnp.sum(squares, axis=0, keepdims=True)
        mine = index * 32 + in_plane
        for c in range(3):
            plane[mine, c : c + 1, :] = total[:, c * 128 : (c + 1) * 128]
            plane[mine, 3 + c : 4 + c, :] = squares[:, c * 128 : (c + 1) * 128]
        norm[index, 2] = jnp.broadcast_to(total * (1.0 / local_count), (8, C))

        for a, b in XY_OFFSETS:
            push(
                plane, mine, plane_s.at[index], plane_r.at[index], **plane_device(a, b), batch_2=HUB
            )

        @pl.when(jnp.logical_not(is_hub))
        def _():
            push(plane, mine, plane_s.at[index], plane_r.at[index], batch_2=HUB)

    def reduce_middle(index):
        @pl.when(is_hub)
        def _():
            wait_bytes(slots(plane, index * 32, 31), plane_r.at[index])
            mine = index * 8 + z
            ring[mine, 0:6] = added(plane, index * 32, 32)
            for d in Z_OFFSETS:
                at = lax.rem(z + d, 8)
                push(ring, mine, ring_s.at[index], ring_r.at[index], batch_2=1 - HUB, rows=at)
                push(ring, mine, ring_s.at[index], ring_r.at[index], rows=at)
            push(ring, mine, ring_s.at[index], ring_r.at[index], batch_2=1 - HUB)

    def reduce_end(index, count):
        @pl.when(is_hub)
        def _():
            wait_bytes(slots(ring, index * 8, 7), ring_r.at[index])

        @pl.when(jnp.logical_not(is_hub))
        def _():
            wait_bytes(slots(ring, index * 8, 8), ring_r.at[index])

        acc = added(ring, index * 8, 8) * (1.0 / count)
        l, n = index // 4, index % 4
        for c in range(3):
            cs = pl.ds(c * 128, 128)
            center = acc[c : c + 1]
            spread = jnp.maximum(acc[3 + c : 4 + c] - center * center, 0.0)
            scale = gain[l, n : n + 1, cs] * lax.rsqrt(spread + EPS)
            shift = bias[l, n : n + 1, cs] - center * scale
            norm[index, 0, :, cs] = jnp.broadcast_to(scale, (8, 128))
            norm[index, 1, :, cs] = jnp.broadcast_to(shift, (8, 128))

    def centred(value, index):
        return flat(tiles(value) - norm[index, 2]).astype(BF16)

    def mean_up(index):
        return (norm.at[index, 2], norm.at[index, 4], 8 + 2 * index)

    def mean_down(index):
        return (norm.at[index, 2], norm.at[index, 3], 9 + 2 * index)

    def scale_shift(index, weight):
        scale, shift = norm[index, 0], norm[index, 1]
        if weight is not None:
            scale, shift = scale * weight, shift * weight
        shift_above = norm[index, 3] * scale + shift
        shift_below = norm[index, 4] * scale + shift
        return scale, shift, shift_above, shift_below

    def affine(value, scale, shift):
        return flat(tiles(value.astype(F32)) * scale + shift)

    def masked_edges(act, last):
        @pl.when(z == 0)
        def _():
            zeroed(act.at[0])

        @pl.when(z == 7)
        def _():
            zeroed(act.at[last])

    def each(n, fn, at_once=1):
        def step(i, _):
            for k in range(at_once):
                fn(i * at_once + k)
            return 0

        lax.fori_loop(0, n // at_once, step, 0)

    def column_pool(load, planes):
        out = []
        for p in range(max(planes // 2, 1)):
            x0, x1 = load(2 * p), load(2 * p + 1)
            x2 = load(2 * p + 2) if 2 * p + 2 < planes else shifted_up(load(0), LOW)
            out.append(jnp.maximum(jnp.maximum(x0, x1), x2))
        return out

    mid_pair = range(2)

    for l in range(LAYERS):
        i0, i1, i2, i3 = (4 * l + n for n in range(4))
        mids = raw_m.at[2 * l]
        fines = raw_f.at[l]
        nexts = raw_m.at[2 * l + 1]
        tops = raw_t.at[l]

        own, up = two(l, 0)

        def join_0(e, act):
            t = tiles(top_in[lax.div(e + 1, 2)]) * up
            for p in mid_pair:
                act[e, p] = flat(silu_of_double(tiles(mid_in[e, p]) * own + t)).astype(BF16)

        if l == 0:

            def place_mid(e):
                out = jnp.dot(perm_m[...], mid_nat[e], preferred_element_type=F32)
                for p in mid_pair:
                    mid_in[e, p] = out[p * K : (p + 1) * K]

            permutation(perm_m, 2, False)
            loads["top"].wait()
            loads["mid"].wait()
            for e in (1, 2):
                top_in[e] = top_nat[e].astype(F32)
            for e in (1, 4):
                place_mid(e)
                join_0(e, act_m)
            send_a[0] = act_m[1]
            send_a[1] = act_m[4]
            entry_round(0)
            up_a = [(send_a.at[0], halo_a.at[1], 6)]
            down_a = [(send_a.at[1], halo_a.at[0], 7)]

            @pl.when(jnp.logical_not(is_hub))
            def _():
                start_sends(up_a, down_a)

            for e in (2, 3):
                place_mid(e)
                join_0(e, act_m)

            @pl.when(is_hub)
            def _():
                start_sends(up_a, down_a)

            sends_up.extend(up_a)
            sends_down.extend(down_a)
            fill_edges()
            entry_round(1)
            spread_taps()
            loads["fine"].wait()
            fine_up = [(fine_nat.at[1], fine_nat.at[9], 4)]
            fine_down = [(fine_nat.at[8], fine_nat.at[0], 5)]
            send(fine_up, fine_down)
            loads["pw"].wait()

            def edge_rows():
                permutation(perm_f, 4, False)
                entry_round(2)
                receive(up_a, down_a)
                act_m[0] = halo_a[0]
                act_m[5] = halo_a[1]

            stats = convolve(act_m, mids, i0, 4, 2, 4, 2, (1, 2, 0, 3), edge_rows)
            entry_round(3)
            entry_end()
        else:
            scale, shift, shift_above, shift_below = scale_shift(3, None)
            for e in range(4):
                if e == 0:
                    top_in[e] = affine(halo_c[0], scale, shift_above)
                elif e == 3:
                    top_in[e] = affine(halo_c[1], scale, shift_below)
                else:
                    top_in[e] = affine(raw_t[0, e - 1, 0], scale, shift)
            each(6, lambda e: join_0(e, act_m), 3)
            masked_edges(act_m, 5)
            stats = convolve(act_m, mids, i0, 4, 2, 4, 2)
        reduce_start(i0, stats, 4 * 96)
        for p in mid_pair:
            send_m[l, 0, p] = centred(mids[0, p], i0)
            send_m[l, 1, p] = centred(mids[3, p], i0)
        up_0 = [(send_m.at[l, 0], halo_m.at[l, 1], 24 + 2 * l), mean_up(i0)]
        down_0 = [(send_m.at[l, 1], halo_m.at[l, 0], 25 + 2 * l), mean_down(i0)]
        send(up_0, down_0)
        if l == 0:
            first_up = [
                (mid_nat.at[1], mid_nat.at[5], 0),
                (top_nat.at[1], top_nat.at[3], 1),
            ]
            first_down = [
                (mid_nat.at[4], mid_nat.at[0], 2),
                (top_nat.at[2], top_nat.at[0], 3),
            ]
            send(first_up, first_down)
        reduce_middle(i0)

        own, up = two(l, 1)
        if l == 0:
            receive(fine_up, fine_down)

            def place_fine(e):
                out = jnp.dot(perm_f[...], fine_nat[e], preferred_element_type=F32)
                for q in range(4):
                    base_f[e, q] = flat(tiles(out[q * K : (q + 1) * K]) * own)

            each(10, place_fine)
            receive(first_up, first_down)
            place_mid(0)
            place_mid(5)
            for e in (0, 3):
                top_in[e] = top_nat[e].astype(F32)
        else:
            receive(up_f, down_f)
            scale, shift, shift_above, shift_below = scale_shift(1, own)

            def place_fine(e):
                for q in range(4):
                    base_f[e + 1, q] = affine(raw_f[0, e, q], scale, shift)

            each(8, place_fine)
            for q in range(4):
                base_f[0, q] = affine(halo_f[0, q], scale, shift_above)
                base_f[9, q] = affine(halo_f[1, q], scale, shift_below)

        receive(up_0, down_0)
        if l == 0:
            for name in ("pw_0", "pw_1", "gain", "bias"):
                loads[name].wait()
        reduce_end(i0, counts[1])

        scale, shift, shift_above, shift_below = scale_shift(i0, up)
        for p in mid_pair:
            lifted[0, p] = affine(halo_m[l, 0, p], scale, shift_above)
            lifted[5, p] = affine(halo_m[l, 1, p], scale, shift_below)

        def lift(e):
            for p in mid_pair:
                lifted[e + 1, p] = affine(mids[e, p], scale, shift)

        each(4, lift, 2)

        def join_1(e):
            m = lax.div(e + 1, 2)
            for p in mid_pair:
                t = lifted[m, p]
                for q in (2 * p, 2 * p + 1):
                    act_f[e, q] = silu_of_double(base_f[e, q] + t).astype(BF16)

        each(10, join_1, 2)
        masked_edges(act_f, 9)
        stats = convolve(act_f, fines, i1, 8, 4, 8, 2)
        reduce_start(i1, stats, 8 * 192)

        def pool_columns(r):
            for p, out in enumerate(column_pool(lambda q: fines[r, q], 4)):
                col_f[r, p] = out

        each(8, pool_columns)
        for p in mid_pair:
            first = jnp.maximum(jnp.maximum(col_f[0, p], col_f[1, p]), col_f[2, p])
            pool_m[1, p] = first
            send_p[l, 0, p] = centred(col_f[0, p], i1)
            send_p[l, 1, p] = centred(first, i1)
            send_p[l, 2, p] = centred(jnp.maximum(col_f[6, p], col_f[7, p]), i1)
        up_1 = [(send_p.at[l, pl.ds(0, 2)], halo_p.at[l, pl.ds(1, 2)], 28 + 2 * l), mean_up(i1)]
        down_1 = [(send_p.at[l, 2], halo_p.at[l, 0], 29 + 2 * l), mean_down(i1)]
        send(up_1, down_1)
        reduce_middle(i1)
        if l == 0:
            for q in range(4):
                send_f[0, q] = centred(fines[0, q], i1)
                send_f[1, q] = centred(fines[7, q], i1)

        w_mid, w_down, w_pool = three(l)
        scale, shift, shift_above, shift_below = scale_shift(i0, w_down)

        def known(e, value, one_shift):
            for p in mid_pair:
                base_m[e, p] = flat(
                    tiles(mid_in[e, p]) * w_mid + tiles(value(p).astype(F32)) * scale + one_shift
                )

        known(0, lambda p: halo_m[l, 0, p], shift_above)
        known(5, lambda p: halo_m[l, 1, p], shift_below)
        each(4, lambda e: known(e + 1, lambda p: mids[e, p], shift))
        w_top, w_up = two(l, 2)
        for e in range(4):
            base_t[e] = flat(tiles(top_in[e]) * w_top)
        for i in (1, 2):
            for p in mid_pair:
                pool_m[i + 1, p] = jnp.maximum(
                    jnp.maximum(col_f[2 * i, p], col_f[2 * i + 1, p]), col_f[2 * i + 2, p]
                )
        receive(up_1, down_1)
        mean_above, mean_below = norm[i1, 3], norm[i1, 4]
        for p in mid_pair:
            pool_m[0, p] = jnp.maximum(
                flat(tiles(halo_p[l, 0, p].astype(F32)) + mean_above), col_f[0, p]
            )
            pool_m[4, p] = jnp.maximum(
                jnp.maximum(col_f[6, p], col_f[7, p]),
                flat(tiles(halo_p[l, 1, p].astype(F32)) + mean_below),
            )
            pool_m[5, p] = flat(tiles(halo_p[l, 2, p].astype(F32)) + mean_below)
        reduce_end(i1, counts[0])

        scale, shift, _, _ = scale_shift(i1, w_pool)

        def join_2(e):
            for p in mid_pair:
                act_m[e, p] = flat(
                    silu_of_double(tiles(base_m[e, p]) + (tiles(pool_m[e, p]) * scale + shift))
                ).astype(BF16)

        each(6, join_2, 3)
        masked_edges(act_m, 5)
        stats = convolve(act_m, nexts, i2, 4, 2, 4, 2)
        reduce_start(i2, stats, 4 * 96)
        for r in range(4):
            col_m[r] = column_pool(lambda q: nexts[r, q], 2)[0]
        first = jnp.maximum(jnp.maximum(col_m[0], col_m[1]), col_m[2])
        pool_t[1] = first
        send_q[l, 0] = centred(col_m[0], i2)
        send_q[l, 1] = centred(first, i2)
        send_q[l, 2] = centred(jnp.maximum(col_m[2], col_m[3]), i2)
        up_2 = [(send_q.at[l, pl.ds(0, 2)], halo_q.at[l, pl.ds(1, 2)], 34 + 2 * l), mean_up(i2)]
        down_2 = [(send_q.at[l, 2], halo_q.at[l, 0], 35 + 2 * l), mean_down(i2)]
        send(up_2, down_2)
        if l == 0:
            for p in mid_pair:
                send_t[0, p] = centred(nexts[0, p], i2)
                send_t[1, p] = centred(nexts[3, p], i2)
            up_t = [(send_t.at[0], halo_t.at[1], 38)]
            down_t = [(send_t.at[1], halo_t.at[0], 39)]
            send(up_t, down_t)
        reduce_middle(i2)
        if l == 1:
            scale, shift, _, _ = scale_shift(i1, None)

            permutation(back_f, 4, True)
            permutation(back_m, 2, True)

            def finish_fine(r):
                for q in range(4):
                    spat[pl.ds(q * K, K), :] = affine(fines[r, q], scale, shift).astype(BF16)
                fine_out[0, r] = jnp.dot(
                    back_f[...], spat[pl.ds(0, 4 * K), :], preferred_element_type=F32
                ).astype(BF16)

            each(8, finish_fine)
        receive(up_2, down_2)
        mean_above, mean_below = norm[i2, 3], norm[i2, 4]
        pool_t[0] = jnp.maximum(flat(tiles(halo_q[l, 0].astype(F32)) + mean_above), col_m[0])
        pool_t[2] = jnp.maximum(
            jnp.maximum(col_m[2], col_m[3]), flat(tiles(halo_q[l, 1].astype(F32)) + mean_below)
        )
        pool_t[3] = flat(tiles(halo_q[l, 2].astype(F32)) + mean_below)
        reduce_end(i2, counts[1])

        scale, shift, _, _ = scale_shift(i2, w_up)
        for e in range(4):
            act_t[e, 0] = flat(
                silu_of_double(tiles(base_t[e]) + (tiles(pool_t[e]) * scale + shift))
            ).astype(BF16)
        masked_edges(act_t, 3)
        stats = convolve(act_t, tops, i3, 2, 1, 2, 2)
        reduce_start(i3, stats, 2 * 48)
        scale, shift, shift_above, shift_below = scale_shift(i2, None)
        if l == 0:
            send_c[0] = centred(tops[0, 0], i3)
            send_c[1] = centred(tops[1, 0], i3)
            up_3 = [(send_c.at[0], halo_c.at[1], 40), mean_up(i3)]
            down_3 = [(send_c.at[1], halo_c.at[0], 41), mean_down(i3)]
            send(up_3, down_3)
            up_f = [(send_f.at[0], halo_f.at[1], 32)]
            down_f = [(send_f.at[1], halo_f.at[0], 33)]
            send(up_f, down_f)
            reduce_middle(i3)
            receive(up_t, down_t)
            for p in mid_pair:
                mid_in[0, p] = affine(halo_t[0, p], scale, shift_above)
                mid_in[5, p] = affine(halo_t[1, p], scale, shift_below)

            def normalize_mid(e):
                for p in mid_pair:
                    mid_in[e + 1, p] = affine(nexts[e, p], scale, shift)

            each(4, normalize_mid)
            receive(up_3, down_3)
            reduce_end(i3, counts[2])
        else:
            reduce_middle(i3)

            def finish_mid(r):
                for p in mid_pair:
                    spat[pl.ds(p * K, K), :] = affine(nexts[r, p], scale, shift).astype(BF16)
                mid_out[0, r] = jnp.dot(
                    back_m[...], spat[pl.ds(0, 2 * K), :], preferred_element_type=F32
                ).astype(BF16)

            each(4, finish_mid)
            reduce_end(i3, counts[2])
            scale, shift, _, _ = scale_shift(i3, None)
            for e in range(2):
                top_out[0, e] = affine(tops[e, 0], scale, shift).astype(BF16)

    @pl.when(has_above)
    def _():
        for src, _, slot in sends_up:
            wait_bytes(src, halo_s.at[slot])

    @pl.when(has_below)
    def _():
        for src, _, slot in sends_down:
            wait_bytes(src, halo_s.at[slot])

    @pl.when(jnp.logical_not(is_hub))
    def _():
        for index in range(8):
            wait_bytes(slots(plane, 0, 16), plane_s.at[index])

    @pl.when(is_hub)
    def _():
        for index in range(8):
            wait_bytes(slots(plane, 0, 15), plane_s.at[index])
            wait_bytes(slots(ring, 0, 15), ring_s.at[index])


def store_kernel(fine, mid, top, fine_out, mid_out, top_out, sems):
    copies = [
        pltpu.make_async_copy(src, dst, sems.at[i])
        for i, (src, dst) in enumerate(((fine, fine_out), (mid, mid_out), (top, top_out)))
    ]
    for copy in copies:
        copy.start()
    for copy in copies:
        copy.wait()


def body(
    fine_level,
    middle_level,
    coarse_level,
    two_input_weights,
    three_input_weights,
    depthwise,
    pointwise,
    bn_gain,
    bn_bias,
):
    devices = lax.axis_size(BATCH) * lax.axis_size("rows")
    counts = tuple(
        float(a.shape[0] * a.shape[1] * a.shape[2] * devices)
        for a in (fine_level, middle_level, coarse_level)
    )
    any_space = pl.BlockSpec(memory_space=pl.ANY)
    smem = pl.BlockSpec(memory_space=pltpu.SMEM)
    vmem = pltpu.VMEM
    dma = pltpu.SemaphoreType.DMA
    scratch = [
        vmem((10, 192, C), BF16),
        vmem((6, 96, C), BF16),
        vmem((4, 48, C), BF16),
        vmem((2, 3, 3, 4, C), BF16),
        vmem((2, 4, C, C), BF16),
        vmem((2, 4, C), F32),
        vmem((2, 4, C), F32),
        vmem((192, 192), BF16),
        vmem((96, 96), BF16),
        vmem((192, 192), BF16),
        vmem((96, 96), BF16),
        vmem((10, 4, K, C), F32),
        vmem((6, 2, K, C), F32),
        vmem((6, 2, K, C), F32),
        vmem((4, K, C), F32),
        vmem((4, K, C), F32),
        vmem((6, 2, K, C), F32),
        vmem((4, 4, 2, K, C), F32),
        vmem((2, 8, 4, K, C), F32),
        vmem((2, 2, 1, K, C), F32),
        vmem((8, 2, K, C), F32),
        vmem((4, K, C), F32),
        vmem((6, 2, K, C), F32),
        vmem((4, K, C), F32),
        vmem((8, 5, 8, C), F32),
        vmem((2, 2, 2, K, C), BF16),
        vmem((2, 2, K, C), BF16),
        vmem((2, 2, K, C), BF16),
        vmem((2, 2, 2, K, C), BF16),
        vmem((2, 3, 2, K, C), BF16),
        vmem((2, 3, 2, K, C), BF16),
        vmem((2, 4, K, C), BF16),
        vmem((2, 4, K, C), BF16),
        vmem((2, 3, K, C), BF16),
        vmem((2, 3, K, C), BF16),
        vmem((2, 2, K, C), BF16),
        vmem((2, 2, K, C), BF16),
        vmem((2, K, C), BF16),
        vmem((2, K, C), BF16),
        vmem((8 * 8, 8, 128), F32),
        vmem((8 * 32, 8, 128), F32),
        dma((9,)),
        dma((8,)),
        dma((8,)),
        dma((8,)),
        dma((8,)),
        dma((42,)),
        dma((42,)),
        pltpu.SemaphoreType.REGULAR((4,)),
    ]
    levels = (fine_level, middle_level, coarse_level)
    results = pl.pallas_call(
        functools.partial(kernel, counts),
        out_shape=tuple(vmem(a.shape, BF16) for a in levels),
        in_specs=[any_space] * 3 + [smem] * 2 + [any_space] * 4,
        out_specs=(pl.BlockSpec(memory_space=vmem),) * 3,
        scratch_shapes=scratch,
        name="bifpn",
        compiler_params=pltpu.CompilerParams(
            collective_id=0, has_side_effects=True, vmem_limit_bytes=60 * 1024 * 1024
        ),
    )(
        fine_level,
        middle_level,
        coarse_level,
        jnp.transpose(two_input_weights, (0, 2, 1)),
        three_input_weights,
        jnp.transpose(depthwise, (0, 2, 3, 1, 4)),
        pointwise,
        bn_gain,
        bn_bias,
    )
    return pl.pallas_call(
        store_kernel,
        out_shape=tuple(jax.ShapeDtypeStruct(a.shape, BF16) for a in levels),
        in_specs=[pl.BlockSpec(memory_space=vmem)] * 3,
        out_specs=(any_space,) * 3,
        scratch_shapes=[dma((3,))],
        name="store",
    )(*(pltpu.with_memory_space_constraint(one, vmem) for one in results))


def solution(mesh):
    split = Mesh(
        mesh.devices.reshape(4, 4, 2, mesh.shape["rows"]), ("batch_0", "batch_1", "batch_2", "rows")
    )
    level = P(BATCH, "rows", None, None)
    return jax.shard_map(
        body,
        mesh=split,
        in_specs=(level,) * 3 + (P(),) * 6,
        out_specs=(level,) * 3,
        check_vma=False,
    )
```
